512 devices in a mesh: dom: 2 (over y), grid: 32 (over z), band: 4 (over x), mem: 2 (over core).
Axes of the slice: x: 4, y: 2, z: 32, core: 2. Of those that a mesh axis runs over, the one named last changes fastest.
The devices are a block of a 4x16x32 slice.
Arguments:
- grid_state: bfloat16 [4, 16384, 128], P(('dom', 'mem'), 'grid'), parts along dimension 0, may hold values from -6 to 6
- forcing: bfloat16 [32768, 128], P(('dom', 'grid')), parts along dimension 0, may hold values from -6 to 6
- boundary_mask: int32 [16384], P('grid'), may hold values 0 or 1
- edge_src: int32 [32, 32, 32], P('grid'), may hold values from 0 to 511
- edge_dst: int32 [32, 32, 32], P(None, 'grid'), may hold values from 0 to 127
- edge_count: int32 [32, 32], P(None, 'grid'), may hold values from 0 to 32, as said below
- edge_weight: float32 [32, 32, 32], P(None, 'grid'), may hold values from 0.1 to 1
- embed_weight: bfloat16 [128, 1024], P(None, 'band'), may hold values from -0.5 to 0.5
- attn_qkv: bfloat16 [1, 1024, 3, 1024], P(None, 'mem', None, 'band'), may hold values from -0.1875 to 0.1875
- attn_out: bfloat16 [1, 1024, 1024], P(None, 'band', 'mem'), may hold values from -0.1875 to 0.1875
- mlp_in: bfloat16 [1, 1024, 4096], P(None, 'mem', 'band'), may hold values from -0.1875 to 0.1875
- mlp_out: bfloat16 [1, 4096, 1024], P(None, 'band', 'mem'), may hold values from -0.09375 to 0.09375
- decode_weight: bfloat16 [1024, 128], P('band'), may hold values from -0.1875 to 0.1875
Outputs:
- next_state: bfloat16 [4, 16384, 128], P(('dom', 'mem'), 'grid'), parts along dimension 0
The draws below stay inside these ranges and needn't reach their ends.
There are 2 independent parts, one for each index of `dom`. The reference program is written for one: setup_inputs(seed, part) draws one part's arguments, and reference() takes and returns one part's arrays. A program takes and returns all parts, laid end to end along the dimension named above; an argument that names none is the same for every part. Nothing has to cross between parts.
Inputs may be any that keep to these rules, and one draw needn't show every extreme that they name: Slots at or beyond edge_count[i, j] in a block are padding. In every draw some mesh band receives 32 live slots from every grid shard.
All inputs are finite; a program needn't handle non-finite values. No bound on the sum of `boundary_mask` on one device may be relied on, other than what follows from the above.
Results may differ from the reference program's by a relative error of at most 0.011.
Values may be sent and summed in bfloat16 or wider, within the bound.
A program may use at most 64 MiB of HBM per device.

```python
import math
import jax
import jax.numpy as jnp
from jax import lax

D = 1024
HEADS = 16
FF = 4096
CHANNELS = 128
LAYERS = 1
GP_DEV = 512
M_DEV = 128
HEAD_DIM = 64
WINDOW = 64
EDGE_SLOTS = 32
MEMBERS = 2
GRID_POINTS = 16384
MESH_NODES = 4096
N_GRID = 32
N_BAND = 4


def draw_edge_count(key, part):
    busiest = jax.random.randint(jax.random.fold_in(key, 7), (), 0, N_GRID)
    counted = jax.random.randint(jax.random.fold_in(key, 11), (N_GRID, N_GRID), 0, EDGE_SLOTS + 1)
    column = jnp.arange(N_GRID, dtype=jnp.int32)[None, :]
    return jnp.where(column == busiest, EDGE_SLOTS, counted).astype(jnp.int32)


def touch_ends(drawn, own_key, least, high):
    spot = [jax.random.randint(jax.random.fold_in(own_key, axis), (), 0, length) for axis, length in enumerate(drawn.shape)]
    main_axis = drawn.shape.index(max(drawn.shape))
    next_to = spot[:main_axis] + [(spot[main_axis] + 1) % drawn.shape[main_axis]] + spot[main_axis + 1:]
    return drawn.at[tuple(spot)].set(least).at[tuple(next_to)].set(high)


def block_levels(own_key, extent, shards, least, high):
    def one(axis_at, parts):
        draws = jax.random.uniform(jax.random.fold_in(jax.random.fold_in(own_key, 6), axis_at), (parts,), jnp.float32, least / len(shards), high / len(shards))
        return jnp.repeat(jnp.exp(draws), extent[axis_at] // parts).reshape((-1,) + (1,) * (len(extent) - axis_at - 1))

    level = one(*shards[0])
    for cut in shards[1:]:
        level = level * one(*cut)
    return level


def noise(own_key, dims, spread, most, cuts=(), kind=jnp.bfloat16):
    values = spread * jax.random.normal(own_key, dims, jnp.float32)
    if cuts:
        values = values * block_levels(own_key, dims, cuts, -0.22, 0.18)
    return jnp.clip(values, -most, most).astype(kind)


def setup_inputs(seed: int = 0, part: int = 0) -> dict:
    key_list = jax.random.split(jax.random.key(seed), 14)
    own_keys = jax.random.split(jax.random.fold_in(key_list[13], part), 14)
    return {
        "grid_state": noise(own_keys[0], (MEMBERS, GRID_POINTS, CHANNELS), 1.0, 6.0, ((0, 2), (1, 32))),
        "forcing": noise(own_keys[1], (GRID_POINTS, CHANNELS), 1.0, 6.0, ((0, 32),)),
        "boundary_mask": touch_ends((jax.random.randint(key_list[2], (GRID_POINTS,), 0, 4) < 1).astype(jnp.int32), jax.random.fold_in(key_list[2], 1), 0, 1),
        "edge_src": touch_ends(jax.random.randint(key_list[3], (N_GRID, N_GRID, EDGE_SLOTS), 0, GP_DEV), jax.random.fold_in(key_list[3], 1), 0, GP_DEV - 1).astype(jnp.int32),
        "edge_dst": touch_ends(jax.random.randint(key_list[4], (N_GRID, N_GRID, EDGE_SLOTS), 0, M_DEV), jax.random.fold_in(key_list[4], 1), 0, M_DEV - 1).astype(jnp.int32),
        "edge_count": draw_edge_count(jax.random.fold_in(key_list[13], 71), part),
        "edge_weight": jnp.clip(jnp.exp(math.log(1.0) - 2.3025851 * jax.random.uniform(key_list[6], (N_GRID, N_GRID, EDGE_SLOTS), jnp.float32) ** block_levels(key_list[6], (N_GRID, N_GRID, EDGE_SLOTS), ((1, 32),), -0.2, 0.2)), 0.1, 1.0),
        "embed_weight": noise(key_list[7], (CHANNELS, D), CHANNELS ** -0.5, 0.5, ((1, 4),)),
        "attn_qkv": noise(key_list[8], (LAYERS, D, 3, D), D ** -0.5, 0.1875, ((1, 2), (3, 4))),
        "attn_out": noise(key_list[9], (LAYERS, D, D), D ** -0.5, 0.1875, ((1, 4), (2, 2))),
        "mlp_in": noise(key_list[10], (LAYERS, D, FF), D ** -0.5, 0.1875, ((1, 2), (2, 4))),
        "mlp_out": noise(key_list[11], (LAYERS, FF, D), FF ** -0.5, 0.09375, ((1, 4), (2, 2))),
        "decode_weight": noise(key_list[12], (D, CHANNELS), D ** -0.5, 0.1875, ((0, 4),)),
    }


def rms_norm(values):
    return values * lax.rsqrt(lax.optimization_barrier(jnp.mean(values * values, axis=-1, keepdims=True)) + 1e-06)

def split_sum(left, right, groups):
    group_span = left.shape[1] // groups
    summed = jnp.zeros((left.shape[0], right.shape[1]), jnp.float32)
    for group_idx in range(groups):
        lower = group_idx * group_span
        partial_value = jnp.dot(left[:, lower:lower + group_span], right[lower:lower + group_span], preferred_element_type=jnp.float32)
        summed = summed + lax.optimization_barrier(partial_value.astype(jnp.bfloat16)).astype(jnp.float32)
    return summed

def encode(grid_rows, edge_src, edge_dst, weights, embed_weight):
    offsets = jnp.arange(N_GRID, dtype=jnp.int32) * M_DEV

    def add_shard(summed, shard):
        rows_here = lax.dynamic_slice_in_dim(grid_rows, shard * GP_DEV, GP_DEV, 0)
        embedded = jax.nn.gelu(jnp.dot(rows_here, embed_weight, preferred_element_type=jnp.float32))
        picked = embedded[edge_src[shard].reshape(-1)] * weights[shard].reshape(-1)[:, None]
        targets = (edge_dst[shard] + offsets[:, None]).reshape(-1)
        return (summed + jax.ops.segment_sum(picked, targets, num_segments=MESH_NODES), None)
    summed, unused = lax.scan(add_shard, jnp.zeros((MESH_NODES, D), jnp.float32), jnp.arange(N_GRID, dtype=jnp.int32))
    return summed

def attend(queries, keys_all, values_all):
    margin = ((WINDOW, WINDOW), (0, 0), (0, 0))
    key_pad = jnp.pad(keys_all, margin)
    value_pad = jnp.pad(values_all, margin)

    def one_block(block):
        start = block * M_DEV
        q_block = lax.dynamic_slice_in_dim(queries, start, M_DEV, 0).astype(jnp.float32)
        k_block = lax.dynamic_slice_in_dim(key_pad, start, M_DEV + 2 * WINDOW, 0).astype(jnp.float32)
        v_block = lax.dynamic_slice_in_dim(value_pad, start, M_DEV + 2 * WINDOW, 0).astype(jnp.float32)
        query_pos = start + jnp.arange(M_DEV, dtype=jnp.int32)
        key_pos = start - WINDOW + jnp.arange(M_DEV + 2 * WINDOW, dtype=jnp.int32)
        visible = (jnp.abs(query_pos[:, None] - key_pos[None, :]) <= WINDOW) & (key_pos[None, :] >= 0) & (key_pos[None, :] < MESH_NODES)
        scores = jnp.einsum('qhd,khd->hqk', q_block, k_block) * HEAD_DIM ** (-0.5)
        exp_scores = jnp.where(visible[None], jnp.exp(scores), 0.0)
        shares = (exp_scores / lax.optimization_barrier(jnp.sum(exp_scores, axis=-1, keepdims=True))).astype(jnp.bfloat16)
        attended = jnp.einsum('hqk,khd->qhd', shares.astype(jnp.float32), v_block)
        return attended.astype(jnp.bfloat16).reshape(M_DEV, D)
    return lax.map(one_block, jnp.arange(N_GRID, dtype=jnp.int32)).reshape(MESH_NODES, D)

def reference(grid_state, forcing, boundary_mask, edge_src, edge_dst, edge_count, edge_weight, embed_weight, attn_qkv, attn_out, mlp_in, mlp_out, decode_weight):
    slot_ids = jnp.arange(EDGE_SLOTS, dtype=jnp.int32)
    live_slot = slot_ids[None, None, :] < edge_count[:, :, None]
    weights = jnp.where(live_slot, edge_weight, jnp.zeros_like(edge_weight))
    src_all = (edge_src + (jnp.arange(N_GRID, dtype=jnp.int32) * GP_DEV)[:, None, None]).reshape(-1)
    dst_all = (edge_dst + (jnp.arange(N_GRID, dtype=jnp.int32) * M_DEV)[None, :, None]).reshape(-1)
    weight_all = weights.reshape(-1)
    results = []
    for member in range(MEMBERS):
        grid_rows = grid_state[member]
        mesh_in = encode(grid_rows, edge_src, edge_dst, weights, embed_weight).astype(jnp.bfloat16)
        stream = mesh_in.astype(jnp.float32)
        for layer_idx in range(LAYERS):
            normed = rms_norm(stream).astype(jnp.bfloat16)
            mixed_qkv = jnp.dot(normed, attn_qkv[layer_idx].reshape(D, 3 * D), preferred_element_type=jnp.float32)
            mixed_qkv = mixed_qkv.reshape(MESH_NODES, 3, HEADS, HEAD_DIM)
            queries = rms_norm(mixed_qkv[:, 0]).astype(jnp.bfloat16)
            keys_all = rms_norm(mixed_qkv[:, 1]).astype(jnp.bfloat16)
            values_all = mixed_qkv[:, 2].astype(jnp.bfloat16)
            attended = attend(queries, keys_all, values_all)
            stream = stream + split_sum(attended, attn_out[layer_idx], N_BAND)
            normed = rms_norm(stream).astype(jnp.bfloat16)
            hidden = jax.nn.gelu(jnp.dot(normed, mlp_in[layer_idx], preferred_element_type=jnp.float32)).astype(jnp.bfloat16)
            stream = stream + split_sum(hidden, mlp_out[layer_idx], N_BAND)
        mesh_out = stream.astype(jnp.bfloat16)
        projected = jnp.dot(mesh_out, decode_weight, preferred_element_type=jnp.float32)
        decoded = jax.ops.segment_sum(projected[dst_all] * weight_all[:, None], src_all, num_segments=GRID_POINTS)
        forced = boundary_mask[:, None] == 1
        result = jnp.where(forced, forcing.astype(jnp.float32), grid_rows.astype(jnp.float32) + decoded)
        results.append(result.astype(jnp.bfloat16))
    return jnp.stack(results)
```

```python
import functools
import math

import jax
import jax.numpy as jnp
from jax import lax
from jax.experimental import pallas as pl
from jax.experimental.pallas import tpu as pltpu
from jax.sharding import PartitionSpec as P

HEADS = 16
M_DEV = 128
WINDOW = 64
EMBED, OUT, DEC, STATE, ATT, MLP, PROJ, BACK = STAGES = range(8)
F32 = jnp.float32
BF16 = jnp.bfloat16
MESH = pl.DeviceIdType.MESH


def dot(left, right):
    return jnp.dot(left, right, preferred_element_type=F32)


def dot_tn(left, right):
    return lax.dot_general(left, right, (((0,), (0,)), ((), ())), preferred_element_type=F32)


def dot_nt(left, right):
    return lax.dot_general(left, right, (((1,), (1,)), ((), ())), preferred_element_type=F32)


def exact_dot(left, right):
    return jnp.dot(left, right, precision=lax.Precision.HIGHEST, preferred_element_type=F32)


def gelu(x):
    return 0.5 * x * (1.0 + jnp.tanh(math.sqrt(2.0 / math.pi) * (x + 0.044715 * (x * x * x))))


def rms_norm(values):
    return values * lax.rsqrt(jnp.mean(values * values, axis=-1, keepdims=True) + 1e-06)


def halves(values):
    high = values.astype(BF16)
    return high, (values - high.astype(F32)).astype(BF16)


def near_first(count, stride, ring):
    return sorted(range(count), key=lambda r: min(stride * r + stride // 2, ring - stride * r - stride // 2))


def step_kernel(
    n_grid, n_band, head_dim,
    grid_in, src_in, dst_in, count_in, weight_in, embed_in, qkv_in, out_in, up_in, down_in, dec_in,
    decoded_ref,
    grid_v, src_v, dst_v, count_v, weight_v, embed_v, qkv_v, out_v, up_v, down_v, dec_v,
    pick, select, send_z, states, near_kv, attended, stream_v, product, pieces, proj, back_z, returned,
    load_sem, z_send, z_recv, x_send, x_recv, mem_send, mem_recv,
):
    me = lax.axis_index("grid")
    band = lax.axis_index("band")
    mem = lax.axis_index("mem")
    other = 1 - mem
    per = n_grid // n_band
    slots = src_v.shape[1]
    group = per * slots
    cls = lax.rem(band - me + n_grid, n_band)
    near = lax.rem(band + 2 * (n_grid - me), n_band)
    own_class, own_place = lax.rem(me, n_band), me // n_band
    is_self = near == 0
    up_next, down_next = lax.rem(me + 1, n_grid), lax.rem(me + n_grid - 1, n_grid)
    bands = [lax.rem(band + q, n_band) for q in range(n_band)]
    far_bands = sorted(range(1, n_band), key=lambda q: -min(q, n_band - q))
    near_bands = far_bands[::-1]
    order = near_first(per, n_band, n_grid)

    def z_peer(r):
        return lax.rem(me + near + n_band * r, n_grid)

    barrier = pltpu.get_barrier_semaphore()

    def greet(device):
        pl.semaphore_signal(barrier, inc=1, device_id=device, device_id_type=MESH)

    for r in order[::-1]:
        if r == 0:
            @pl.when(jnp.logical_not(is_self))
            def _():
                greet({"grid": z_peer(0)})
        else:
            greet({"grid": z_peer(r)})
    greet({"grid": up_next})
    greet({"grid": down_next})
    for q in far_bands:
        greet({"band": bands[q]})
    greet({"mem": other})

    loads = [
        pltpu.make_async_copy(source, target, load_sem.at[k])
        for k, (source, target) in enumerate(
            (
                (src_in, src_v), (dst_in, dst_v), (count_in, count_v), (weight_in, weight_v), (grid_in, grid_v),
                (embed_in, embed_v.at[band]), (qkv_in, qkv_v.at[mem]), (out_in, out_v.at[band, mem]),
                (up_in, up_v.at[mem]), (down_in, down_v.at[mem]), (dec_in, dec_v.at[band]),
            )
        )
    ]
    for load in loads:
        load.start()
    for load in loads[:5]:
        load.wait()

    slot_of = lax.broadcasted_iota(jnp.int32, (slots, group), 1)
    spread = jnp.where(lax.rem(slot_of, slots) == lax.broadcasted_iota(jnp.int32, (slots, group), 0), 1.0, 0.0).astype(F32)
    shard_row = lax.broadcasted_iota(jnp.int32, (n_grid, group), 0)
    place_lane = lax.broadcasted_iota(jnp.int32, (n_grid, group), 1) // slots
    square_row = lax.broadcasted_iota(jnp.int32, (n_grid, n_grid), 0)
    square_lane = lax.broadcasted_iota(jnp.int32, (n_grid, n_grid), 1)
    counts = jnp.sum(
        jnp.where(square_row == square_lane, count_v[...].astype(F32), 0.0), axis=1, keepdims=True
    )
    slot_lane = lax.broadcasted_iota(jnp.int32, (n_grid, slots), 1).astype(F32)
    live = jnp.where(slot_lane < counts, weight_v[:, 0, :], 0.0)
    src_wide = exact_dot(src_v[...].astype(F32), spread)
    dst_wide = exact_dot(dst_v[:, 0, :].astype(F32), spread)
    live_wide = exact_dot(live, spread)

    def lane_row(wide, c):
        return jnp.sum(jnp.where(shard_row == c + n_band * place_lane, wide, 0.0), axis=0, keepdims=True)

    def build_pick(c):
        point = lax.broadcasted_iota(jnp.int32, (grid_v.shape[0], group), 0).astype(F32)
        pick[c] = jnp.where(point == lane_row(src_wide, c), 1.0, 0.0).astype(BF16)

    def build_select(c):
        rows = stream_v.shape[0]
        node = lax.broadcasted_iota(jnp.int32, (rows, group), 0).astype(F32)
        table = jnp.where(node == lane_row(dst_wide, c), lane_row(live_wide, c), 0.0)
        high, low = halves(table)
        select[c, 0:rows] = high
        select[c, rows : 2 * rows] = low

    build_pick(cls)
    send_z[...] = dot_tn(pick[cls], grid_v[...]).astype(BF16).reshape(send_z.shape)
    for c in range(n_band):
        build_select(c)
    for load in loads[5:]:
        load.wait()

    pl.semaphore_wait(barrier, per + 2 + n_band - jnp.where(is_self, 1, 0))

    def z_copy(way, r, source, target):
        peer = z_peer(r)
        return pltpu.make_async_remote_copy(
            src_ref=source.at[peer // n_band], dst_ref=target.at[own_class, own_place],
            send_sem=z_send.at[way, r], recv_sem=z_recv.at[way, own_place],
            device_id={"grid": peer}, device_id_type=MESH,
        )

    def z_arrival(way, r, source, target):
        peer = z_peer(r)
        return pltpu.make_async_remote_copy(
            src_ref=source.at[peer // n_band], dst_ref=target.at[cls, peer // n_band],
            send_sem=z_send.at[way, r], recv_sem=z_recv.at[way, peer // n_band],
            device_id={"grid": peer}, device_id_type=MESH,
        )

    def z_own(way, source, target):
        return pltpu.make_async_copy(source.at[own_place], target.at[cls, own_place], z_recv.at[way, own_place])

    def z_start(way, source, target):
        for r in order[::-1]:
            if r == 0:
                @pl.when(is_self)
                def _():
                    z_own(way, source, target).start()

                @pl.when(jnp.logical_not(is_self))
                def _():
                    z_copy(way, 0, source, target).start()
            else:
                z_copy(way, r, source, target).start()

    def z_wait(way, r, source, target):
        if r == 0:
            @pl.when(is_self)
            def _():
                z_own(way, source, target).wait()

            @pl.when(jnp.logical_not(is_self))
            def _():
                z_arrival(way, 0, source, target).wait_recv()
        else:
            z_arrival(way, r, source, target).wait_recv()

    def z_sent(way, source, target):
        for r in order:
            if r == 0:
                @pl.when(jnp.logical_not(is_self))
                def _():
                    z_copy(way, 0, source, target).wait_send()
            else:
                z_copy(way, r, source, target).wait_send()

    def x_copy(stage, q, source, target):
        return pltpu.make_async_remote_copy(
            src_ref=source, dst_ref=target, send_sem=x_send.at[stage, q], recv_sem=x_recv.at[stage, n_band - q],
            device_id={"band": bands[q]}, device_id_type=MESH,
        )

    def x_wait(stage, q, target):
        pltpu.make_async_remote_copy(
            src_ref=target, dst_ref=target, send_sem=x_send.at[stage, q], recv_sem=x_recv.at[stage, q],
            device_id={"band": bands[q]}, device_id_type=MESH,
        ).wait_recv()

    def mem_copy(k, source, target):
        return pltpu.make_async_remote_copy(
            src_ref=source, dst_ref=target, send_sem=mem_send.at[k], recv_sem=mem_recv.at[k],
            device_id={"mem": other}, device_id_type=MESH,
        )


    def gather_start(stage, ref, index):
        copies = [x_copy(stage, q, ref.at[index], ref.at[index]) for q in far_bands]
        for copy in copies:
            copy.start()
        return copies

    z_start(0, send_z, states)
    sent = gather_start(EMBED, embed_v, band)
    shared = [
        mem_copy(0, qkv_v.at[mem], qkv_v.at[mem]),
        mem_copy(1, up_v.at[mem], up_v.at[mem]),
        mem_copy(2, down_v.at[mem], down_v.at[mem]),
        mem_copy(3, out_v.at[band, mem], out_v.at[band, mem]),
    ]
    for copy in shared:
        copy.start()
    out_sent = [x_copy(OUT, q, out_v.at[band, mem], out_v.at[band, mem]) for q in far_bands]
    for copy in out_sent:
        copy.start()
    sent += out_sent

    for c in range(n_band):
        @pl.when(c != cls)
        def _():
            build_pick(c)

    def pass_on(r, ref, stage):
        place = z_peer(r) // n_band
        for q in far_bands:
            x_copy(stage, q, ref.at[cls, place], ref.at[cls, place]).start()

    for r in order:
        z_wait(0, r, send_z, states)
        pass_on(r, states, STATE)
    sent += gather_start(DEC, dec_v, band)

    rows = stream_v.shape[0]
    width = embed_v.shape[2]
    for q in near_bands:
        x_wait(EMBED, q, embed_v.at[bands[q]])
    for q in [0] + near_bands:
        c = lax.rem(cls + q, n_band)
        if q:
            x_wait(STATE, q, states.at[c])
        block = states[c].reshape(group, -1)
        for col in range(n_band):
            latent = gelu(dot(block, embed_v[col])).astype(BF16)
            both = dot(select[c], latent)
            part = both[:rows] + both[rows:]
            cols = slice(col * width, (col + 1) * width)
            stream_v[:, cols] = part if q == 0 else stream_v[:, cols] + part
    stream = stream_v[...].astype(BF16).astype(F32)
    normed = rms_norm(stream).astype(BF16)

    mem_copy(0, qkv_v.at[other], qkv_v.at[other]).wait_recv()
    deep = qkv_v.shape[2]

    def project(which):
        return dot(normed[:, :deep], qkv_v[0, which]) + dot(normed[:, deep:], qkv_v[1, which])

    lane_r = lax.broadcasted_iota(jnp.int32, (width, width), 0) // head_dim
    lane_c = lax.broadcasted_iota(jnp.int32, (width, width), 1) // head_dim
    head_mean = jnp.where(lane_r == lane_c, 1.0 / head_dim, 0.0).astype(BF16)

    def head_norm(values):
        high, low = halves(values * values)
        return values * lax.rsqrt(dot(high, head_mean) + dot(low, head_mean) + 1e-06)

    near_kv[0:rows, 0:width] = head_norm(project(1)).astype(BF16)
    near_kv[0:rows, width:] = project(2).astype(BF16)
    lower, upper = pl.ds(rows, WINDOW), pl.ds(rows + WINDOW, WINDOW)

    def halo(k, source, target, device):
        return pltpu.make_async_remote_copy(
            src_ref=near_kv.at[source], dst_ref=near_kv.at[target], send_sem=mem_send.at[k], recv_sem=mem_recv.at[k],
            device_id={"grid": device}, device_id_type=MESH,
        )

    n_shared = 4 + n_band - 1
    to_next = halo(n_shared, pl.ds(rows - WINDOW, WINDOW), lower, up_next)
    to_last = halo(n_shared + 1, pl.ds(0, WINDOW), upper, down_next)
    to_next.start()
    to_last.start()

    for q in near_bands:
        x_wait(OUT, q, out_v.at[bands[q], mem])
        copy = mem_copy(3 + q, out_v.at[bands[q], mem], out_v.at[bands[q], mem])
        copy.start()
        shared.append(copy)

    n_heads = width // head_dim
    query = head_norm(project(0)).astype(BF16) * jnp.asarray(head_dim**-0.5, BF16)
    head_lane = lax.broadcasted_iota(jnp.int32, (rows, width), 1) // head_dim
    zero = jnp.zeros_like(query)
    heads = jnp.concatenate([jnp.where(head_lane == h, query, zero) for h in range(n_heads)], axis=0)
    tall = n_heads * rows
    q_pos = lax.rem(lax.broadcasted_iota(jnp.int32, (tall, rows), 0), rows)
    k_pos = lax.broadcasted_iota(jnp.int32, (tall, rows), 1)
    own_scores = dot_nt(heads, near_kv[0:rows, 0:width])
    own_exp = jnp.where(jnp.abs(q_pos - k_pos) <= WINDOW, jnp.exp(own_scores), 0.0)
    to_next.wait()
    to_last.wait()
    far_pos = jnp.where(k_pos < WINDOW, k_pos - WINDOW, k_pos + rows - WINDOW)
    first, last = me == 0, me == n_grid - 1
    low_pos = jnp.where(first, 0, -WINDOW)
    high_pos = jnp.where(last, rows, rows + WINDOW)
    far_ok = (jnp.abs(q_pos - far_pos) <= WINDOW) & (far_pos >= low_pos) & (far_pos < high_pos)
    far_exp = jnp.where(far_ok, jnp.exp(dot_nt(heads, near_kv[rows:, 0:width])), 0.0)
    total = jnp.sum(own_exp, axis=-1, keepdims=True) + jnp.sum(far_exp, axis=-1, keepdims=True)
    mixed = dot((own_exp / total).astype(BF16), near_kv[0:rows, width:])
    mixed += dot((far_exp / total).astype(BF16), near_kv[rows:, width:])
    joined = mixed[0:rows]
    for h in range(1, n_heads):
        joined = jnp.where(head_lane == h, mixed[h * rows : (h + 1) * rows], joined)
    attended[band] = joined.astype(BF16)
    sent += gather_start(ATT, attended, band)

    half = out_v.shape[3]
    mem_copy(3, out_v.at[band, other], out_v.at[band, other]).wait_recv()
    sums = [0.0, 0.0]
    for q in [0] + near_bands:
        if q:
            x_wait(ATT, q, attended.at[bands[q]])
            mem_copy(3 + q, out_v.at[bands[q], other], out_v.at[bands[q], other]).wait_recv()
        left = attended[bands[q]]
        for m in range(2):
            sums[m] = sums[m] + dot(left, out_v[bands[q], m]).astype(BF16).astype(F32)
    stream = stream + jnp.concatenate(sums, axis=1)
    stream_v[...] = stream
    normed = rms_norm(stream).astype(BF16)

    mem_copy(1, up_v.at[other], up_v.at[other]).wait_recv()
    mem_copy(2, down_v.at[other], down_v.at[other]).wait_recv()
    deep = up_v.shape[1]
    hidden = gelu(dot(normed[:, :deep], up_v[0]) + dot(normed[:, deep:], up_v[1])).astype(BF16)
    for m in range(2):
        product[:, m * half : (m + 1) * half] = dot(hidden, down_v[m]).astype(BF16)

    share = rows // n_band
    for q in far_bands:
        copy = x_copy(MLP, q, product.at[pl.ds(pl.multiple_of(bands[q] * share, share), share)], pieces.at[q])
        copy.start()
        sent.append(copy)
    own_rows = pl.ds(pl.multiple_of(band * share, share), share)
    stream = stream_v[own_rows] + product[own_rows].astype(F32)
    for q in near_bands:
        x_wait(DEC, q, dec_v.at[bands[q]])
    for q in near_bands:
        x_wait(MLP, q, pieces.at[n_band - q])
        stream = stream + pieces[n_band - q].astype(F32)
    mesh_out = stream.astype(BF16)
    decoded = dot(mesh_out[:, :width], dec_v[0])
    for k in range(1, n_band):
        decoded += dot(mesh_out[:, k * width : (k + 1) * width], dec_v[k])
    proj[band] = decoded.astype(BF16)
    sent += gather_start(PROJ, proj, band)
    for q in near_bands:
        x_wait(PROJ, q, proj.at[bands[q]])

    nodes = proj[...].reshape(rows, -1)
    z_sent(0, send_z, states)
    outgoing = dot_tn(select[cls, 0:rows], nodes) + dot_tn(select[cls, rows : 2 * rows], nodes)
    back_z[...] = outgoing.astype(BF16).reshape(back_z.shape)
    z_start(1, back_z, returned)

    for q in far_bands:
        x_copy(STATE, q, states.at[cls], states.at[cls]).wait_send()
    for copy in sent + shared:
        copy.wait_send()

    for r in order:
        z_wait(1, r, back_z, returned)
        pass_on(r, returned, BACK)
    decoded_ref[...] = dot(pick[cls], returned[cls].reshape(group, -1))
    for q in near_bands:
        c = lax.rem(cls + q, n_band)
        x_wait(BACK, q, returned.at[c])
        decoded_ref[...] += dot(pick[c], returned[c].reshape(group, -1))
    z_sent(1, back_z, returned)
    for q in far_bands:
        x_copy(BACK, q, returned.at[cls], returned.at[cls]).wait_send()


def body(
    grid_state, forcing, boundary_mask, edge_src, edge_dst, edge_count, edge_weight,
    embed_weight, attn_qkv, attn_out, mlp_in, mlp_out, decode_weight,
):
    n_grid, n_band, n_mem = lax.axis_size("grid"), lax.axis_size("band"), lax.axis_size("mem")
    grid_rows = grid_state[0]
    points, channels = grid_rows.shape
    slots = edge_src.shape[2]
    model = decode_weight.shape[0] * n_band
    width = embed_weight.shape[1]
    rows = M_DEV
    per = n_grid // n_band
    group = per * slots
    operands = (
        grid_rows, edge_src[0], edge_dst, edge_count.T, edge_weight, embed_weight,
        jnp.swapaxes(attn_qkv[0], 0, 1), attn_out[0], mlp_in[0], mlp_out[0], decode_weight,
    )
    vmem = pltpu.VMEM
    scratch = [
        vmem(operands[0].shape, BF16),
        vmem(operands[1].shape, jnp.int32),
        vmem(operands[2].shape, jnp.int32),
        vmem(operands[3].shape, jnp.int32),
        vmem(operands[4].shape, F32),
        vmem((n_band, *operands[5].shape), BF16),
        vmem((n_mem, *operands[6].shape), BF16),
        vmem((n_band, n_mem, *operands[7].shape), BF16),
        vmem((n_mem, *operands[8].shape), BF16),
        vmem((n_mem, *operands[9].shape), BF16),
        vmem((n_band, *operands[10].shape), BF16),
        vmem((n_band, points, group), BF16),
        vmem((n_band, 2 * rows, group), BF16),
        vmem((per, slots, channels), BF16),
        vmem((n_band, per, slots, channels), BF16),
        vmem((rows + 2 * WINDOW, 2 * width), BF16),
        vmem((n_band, rows, width), BF16),
        vmem((rows, model), F32),
        vmem((rows, model), BF16),
        vmem((n_band, rows // n_band, model), BF16),
        vmem((n_band, rows // n_band, channels), BF16),
        vmem((per, slots, channels), BF16),
        vmem((n_band, per, slots, channels), BF16),
        pltpu.SemaphoreType.DMA((11,)),
        pltpu.SemaphoreType.DMA((2, per)),
        pltpu.SemaphoreType.DMA((2, per)),
        pltpu.SemaphoreType.DMA((len(STAGES), n_band)),
        pltpu.SemaphoreType.DMA((len(STAGES), n_band)),
        pltpu.SemaphoreType.DMA((n_band + 5,)),
        pltpu.SemaphoreType.DMA((n_band + 5,)),
    ]
    decoded = pl.pallas_call(
        functools.partial(step_kernel, n_grid, n_band, model // HEADS),
        out_shape=jax.ShapeDtypeStruct((points, channels), F32),
        in_specs=[pl.BlockSpec(memory_space=pl.ANY)] * len(operands),
        out_specs=pl.BlockSpec(memory_space=pltpu.VMEM),
        scratch_shapes=scratch,
        compiler_params=pltpu.CompilerParams(collective_id=0, has_side_effects=True),
    )(*operands)
    forced = boundary_mask[:, None] == 1
    result = jnp.where(forced, forcing.astype(F32), grid_rows.astype(F32) + decoded)
    return result.astype(BF16)[None]


def solution(mesh):
    return jax.shard_map(
        body,
        mesh=mesh,
        in_specs=(
            P(("dom", "mem"), "grid", None),
            P(("dom", "grid"), None),
            P("grid"),
            P("grid", None, None),
            P(None, "grid", None),
            P(None, "grid"),
            P(None, "grid", None),
            P(None, "band"),
            P(None, "mem", None, "band"),
            P(None, "band", "mem"),
            P(None, "mem", "band"),
            P(None, "band", "mem"),
            P("band", None),
        ),
        out_specs=P(("dom", "mem"), "grid", None),
        check_vma=False,
    )
```

```python
import functools
import math

import jax
import jax.numpy as jnp
from jax import lax
from jax.experimental import pallas as pl
from jax.experimental.pallas import tpu as pltpu
from jax.sharding import PartitionSpec as P

HEADS = 16
M_DEV = 128
WINDOW = 64
EMBED, OUT, PASS, DEC, ATT, PROJ, *MORE = STAGES = range(10)
STATES, BACKS = MORE[:2], MORE[2:]
F32 = jnp.float32
BF16 = jnp.bfloat16
MESH = pl.DeviceIdType.MESH


def dot(left, right):
    return jnp.dot(left, right, preferred_element_type=F32)


def dot_tn(left, right):
    return lax.dot_general(left, right, (((0,), (0,)), ((), ())), preferred_element_type=F32)


def dot_nt(left, right):
    return lax.dot_general(left, right, (((1,), (1,)), ((), ())), preferred_element_type=F32)


def exact_dot(left, right):
    return jnp.dot(left, right, precision=lax.Precision.HIGHEST, preferred_element_type=F32)


def gelu(x):
    return 0.5 * x * (1.0 + jnp.tanh(math.sqrt(2.0 / math.pi) * (x + 0.044715 * (x * x * x))))


def rms_norm(values):
    return values * lax.rsqrt(jnp.mean(values * values, axis=-1, keepdims=True) + 1e-06)


def halves(values):
    high = values.astype(BF16)
    return high, (values - high.astype(F32)).astype(BF16)


def near_first(count, stride, ring):
    return sorted(range(count), key=lambda r: min(stride * r + stride // 2, ring - stride * r - stride // 2))


def step_kernel(
    n_grid, n_band, head_dim,
    grid_in, forcing_in, mask_in, src_in, dst_in, count_in, weight_in, embed_in, qkv_in, out_in, up_in, down_in, dec_in,
    next_ref,
    grid_v, forcing_v, mask_v, src_v, dst_v, count_v, weight_v, embed_v, qkv_v, out_v, up_v, down_v, dec_v,
    pick, select, free_v, send_z, states, near_kv, attended, stream_v, fold_v, proj, back_z, returned,
    load_sem, z_send, z_recv, x_send, x_recv, mem_send, mem_recv,
):
    me = lax.axis_index("grid")
    band = lax.axis_index("band")
    mem = lax.axis_index("mem")
    other = 1 - mem
    per = n_grid // n_band
    slots = src_v.shape[1]
    group = per * slots
    up_next, down_next = lax.rem(me + 1, n_grid), lax.rem(me + n_grid - 1, n_grid)
    bands = [lax.rem(band + q, n_band) for q in range(n_band)]
    far_bands = sorted(range(1, n_band), key=lambda q: -min(q, n_band - q))
    near_bands = far_bands[::-1]
    beside, across = (1, n_band - 1), n_band // 2
    order = near_first(per, n_band, n_grid)
    place_of = {r: p for p, r in enumerate(order)}
    near = [lax.rem(bands[q] + 2 * (n_grid - me), n_band) for q in range(n_band)]
    is_self = near[0] == 0

    def z_peer(p):
        return lax.rem(me + near[0] + n_band * order[p], n_grid)

    def place_there(p):
        r = order[p]
        return jnp.where(is_self, place_of[(per - r) % per], place_of[per - 1 - r])

    barrier = pltpu.get_barrier_semaphore()

    def greet(device):
        pl.semaphore_signal(barrier, inc=1, device_id=device, device_id_type=MESH)

    for p in range(per)[::-1]:
        if order[p] == 0:
            @pl.when(jnp.logical_not(is_self))
            def _():
                greet({"grid": z_peer(p)})
        else:
            greet({"grid": z_peer(p)})
    greet({"grid": up_next})
    greet({"grid": down_next})
    for q in far_bands:
        greet({"band": bands[q]})
    greet({"mem": other})

    half = dec_v.shape[2]
    loads = [
        pltpu.make_async_copy(source, target, load_sem.at[k])
        for k, (source, target) in enumerate(
            (
                (src_in, src_v), (grid_in, grid_v), (embed_in, embed_v.at[band]),
                (dst_in, dst_v), (count_in, count_v), (weight_in, weight_v), (mask_in, mask_v), (forcing_in, forcing_v),
                (qkv_in, qkv_v.at[mem]), (out_in, out_v.at[band, mem]), (up_in, up_v.at[mem]), (down_in, down_v.at[mem]),
                (dec_in.at[0:half], dec_v.at[band, 0]), (dec_in.at[half : 2 * half], dec_v.at[band, 1]),
            )
        )
    ]
    for load in loads:
        load.start()

    lane = lax.broadcasted_iota(jnp.int32, (slots, group), 1)
    spread = jnp.where(lax.rem(lane, slots) == lax.broadcasted_iota(jnp.int32, (slots, group), 0), 1.0, 0.0).astype(F32)
    shard_row = lax.broadcasted_iota(jnp.int32, (n_grid, group), 0)
    place_lane = lax.broadcasted_iota(jnp.int32, (n_grid, group), 1) // slots
    step_lane = jnp.zeros_like(place_lane)
    for p in range(per):
        step_lane = jnp.where(place_lane == p, n_band * order[p], step_lane)

    def lane_row(wide, q):
        mine = shard_row == lax.rem(step_lane + (me + near[q]), n_grid)
        return jnp.sum(jnp.where(mine, wide, 0.0), axis=0, keepdims=True)

    def build_pick(q):
        point = lax.broadcasted_iota(jnp.int32, (grid_v.shape[0], group), 0).astype(F32)
        pick[q] = jnp.where(point == lane_row(src_wide, q), 1.0, 0.0).astype(BF16)

    with jax.named_scope("w_load"):
        loads[0].wait()
        loads[1].wait()
    src_wide = exact_dot(src_v[...].astype(F32), spread)
    build_pick(0)
    send_z[...] = dot_tn(pick[0], grid_v[...]).astype(BF16).reshape(send_z.shape)

    with jax.named_scope("w_barrier"):
        pl.semaphore_wait(barrier, per + 2 + n_band - jnp.where(is_self, 1, 0))

    def z_copy(way, p, source, target):
        there = place_there(p)
        return pltpu.make_async_remote_copy(
            src_ref=source.at[p], dst_ref=target.at[0, there], send_sem=z_send.at[way, p], recv_sem=z_recv.at[way, there],
            device_id={"grid": z_peer(p)}, device_id_type=MESH,
        )

    def z_arrival(way, p, source, target):
        return pltpu.make_async_remote_copy(
            src_ref=source.at[p], dst_ref=target.at[0, p], send_sem=z_send.at[way, p], recv_sem=z_recv.at[way, p],
            device_id={"grid": z_peer(p)}, device_id_type=MESH,
        )

    def z_own(way, p, source, target):
        return pltpu.make_async_copy(source.at[p], target.at[0, p], z_recv.at[way, p])

    def z_start(way, source, target):
        for p in range(per)[::-1]:
            if order[p] == 0:
                @pl.when(is_self)
                def _():
                    z_own(way, p, source, target).start()

                @pl.when(jnp.logical_not(is_self))
                def _():
                    z_copy(way, p, source, target).start()
            else:
                z_copy(way, p, source, target).start()

    def z_wait(way, p, source, target):
        if order[p] == 0:
            @pl.when(is_self)
            def _():
                z_own(way, p, source, target).wait()

            @pl.when(jnp.logical_not(is_self))
            def _():
                z_arrival(way, p, source, target).wait_recv()
        else:
            z_arrival(way, p, source, target).wait_recv()

    def z_sent(way, source, target):
        for p in range(per):
            if order[p] == 0:
                @pl.when(jnp.logical_not(is_self))
                def _():
                    z_copy(way, p, source, target).wait_send()
            else:
                z_copy(way, p, source, target).wait_send()

    def x_copy(stage, q, source, target):
        return pltpu.make_async_remote_copy(
            src_ref=source, dst_ref=target, send_sem=x_send.at[stage, q], recv_sem=x_recv.at[stage, n_band - q],
            device_id={"band": bands[q]}, device_id_type=MESH,
        )

    def x_wait(stage, q, target):
        pltpu.make_async_remote_copy(
            src_ref=target, dst_ref=target, send_sem=x_send.at[stage, q], recv_sem=x_recv.at[stage, q],
            device_id={"band": bands[q]}, device_id_type=MESH,
        ).wait_recv()

    def mem_copy(k, ref):
        return pltpu.make_async_remote_copy(
            src_ref=ref, dst_ref=ref, send_sem=mem_send.at[k], recv_sem=mem_recv.at[k],
            device_id={"mem": other}, device_id_type=MESH,
        )

    sent = []

    def start(copy):
        copy.start()
        sent.append(copy)

    def gather_start(stage, ref):
        for q in far_bands:
            start(x_copy(stage, q, ref, ref))

    QKV, UP, DOWN, OUT_OWN, DEC_OWN, LOW, HIGH = 0, 1, 2, 3, 3 + n_band, 3 + 2 * n_band, 4 + 2 * n_band

    z_start(0, send_z, states)
    with jax.named_scope("w_load2"):
        loads[2].wait()
    gather_start(EMBED, embed_v.at[band])
    with jax.named_scope("w_load3"):
        for load in loads[3:]:
            load.wait()
    for k, ref in ((QKV, qkv_v), (UP, up_v), (DOWN, down_v)):
        start(mem_copy(k, ref.at[mem]))
    start(mem_copy(OUT_OWN, out_v.at[band, mem]))

    rows = stream_v.shape[0]
    square_row = lax.broadcasted_iota(jnp.int32, (n_grid, n_grid), 0)
    square_lane = lax.broadcasted_iota(jnp.int32, (n_grid, n_grid), 1)
    counts = jnp.sum(jnp.where(square_row == square_lane, count_v[...].astype(F32), 0.0), axis=1, keepdims=True)
    slot_lane = lax.broadcasted_iota(jnp.int32, (n_grid, slots), 1).astype(F32)
    live = jnp.where(slot_lane < counts, weight_v[:, 0, :], 0.0)
    dst_wide = exact_dot(dst_v[:, 0, :].astype(F32), spread)
    live_wide = exact_dot(live, spread)
    node = lax.broadcasted_iota(jnp.int32, (rows, group), 0).astype(F32)
    for q in range(n_band):
        table = jnp.where(node == lane_row(dst_wide, q), lane_row(live_wide, q), 0.0)
        high, low = halves(table)
        select[q, 0:rows] = high
        select[q, rows : 2 * rows] = low
    for q in range(1, n_band):
        build_pick(q)
    lanes = mask_v.shape[1]
    diagonal = lax.broadcasted_iota(jnp.int32, (lanes, lanes), 0) == lax.broadcasted_iota(jnp.int32, (lanes, lanes), 1)
    for k in range(mask_v.shape[0]):
        flags = jnp.where(mask_v[k : k + 1, :] == 1, 0.0, 1.0).astype(F32)
        column = jnp.sum(jnp.where(diagonal, flags, 0.0), axis=1, keepdims=True)
        free_v[k * lanes : (k + 1) * lanes] = jnp.broadcast_to(column, (lanes, free_v.shape[1]))

    near_part = per // 2
    parts = (slice(0, near_part), slice(near_part, per))

    def pass_on(p, ref, stages):
        for q in far_bands:
            x_copy(stages[p // near_part], q, ref.at[0, p], ref.at[n_band - q, p]).start()

    def passed_on(ref, stages):
        for k, part in enumerate(parts):
            for q in far_bands:
                x_copy(stages[k], q, ref.at[0, part], ref.at[n_band - q, part]).wait_send()

    width = embed_v.shape[2]

    def encode(k, q, first):
        span = near_part * slots
        block = states[q, parts[k]].reshape(span, -1)
        table = select[q, :, k * span : (k + 1) * span]
        for col in range(n_band):
            both = dot(table, gelu(dot(block, embed_v[col])).astype(BF16))
            part = both[:rows] + both[rows:]
            cols = slice(col * width, (col + 1) * width)
            stream_v[:, cols] = part if first else stream_v[:, cols] + part

    with jax.named_scope("w_znear"):
        for p in range(near_part):
            z_wait(0, p, send_z, states)
            pass_on(p, states, STATES)
    with jax.named_scope("w_embed"):
        for q in near_bands:
            x_wait(EMBED, q, embed_v.at[bands[q]])
    encode(0, 0, True)
    with jax.named_scope("w_zfar"):
        for p in range(near_part, per):
            z_wait(0, p, send_z, states)
            pass_on(p, states, STATES)
    for q in far_bands:
        start(x_copy(DEC, q, dec_v.at[band, mem], dec_v.at[band, mem]))
    for q in beside:
        start(x_copy(OUT, q, out_v.at[band, mem], out_v.at[band, mem]))
    encode(1, 0, False)
    for k in range(2):
        for q in near_bands:
            with jax.named_scope(f"w_x{k}{q}"):
                x_wait(STATES[k], q, states.at[q, parts[k]])
            encode(k, q, False)
    stream = stream_v[...].astype(BF16).astype(F32)
    stream_v[...] = stream
    normed = rms_norm(stream).astype(BF16)

    with jax.named_scope("w_qkv"):
        mem_copy(QKV, qkv_v.at[other]).wait_recv()
    deep = qkv_v.shape[2]

    def project(which):
        return dot(normed[:, :deep], qkv_v[0, which]) + dot(normed[:, deep:], qkv_v[1, which])

    lane_r = lax.broadcasted_iota(jnp.int32, (width, width), 0) // head_dim
    lane_c = lax.broadcasted_iota(jnp.int32, (width, width), 1) // head_dim
    head_mean = jnp.where(lane_r == lane_c, 1.0 / head_dim, 0.0).astype(BF16)

    def head_norm(values):
        high, low = halves(values * values)
        return values * lax.rsqrt(dot(high, head_mean) + dot(low, head_mean) + 1e-06)

    near_kv[0:rows, 0:width] = head_norm(project(1)).astype(BF16)
    near_kv[0:rows, width:] = project(2).astype(BF16)
    lower, upper = pl.ds(rows, WINDOW), pl.ds(rows + WINDOW, WINDOW)

    def halo(k, source, target, device):
        return pltpu.make_async_remote_copy(
            src_ref=near_kv.at[source], dst_ref=near_kv.at[target], send_sem=mem_send.at[k], recv_sem=mem_recv.at[k],
            device_id={"grid": device}, device_id_type=MESH,
        )

    to_next = halo(LOW, pl.ds(rows - WINDOW, WINDOW), lower, up_next)
    to_last = halo(HIGH, pl.ds(0, WINDOW), upper, down_next)
    to_next.start()
    to_last.start()

    n_heads = width // head_dim
    query = head_norm(project(0)).astype(BF16) * jnp.asarray(head_dim**-0.5, BF16)
    head_lane = lax.broadcasted_iota(jnp.int32, (rows, width), 1) // head_dim
    zero = jnp.zeros_like(query)
    heads = jnp.concatenate([jnp.where(head_lane == h, query, zero) for h in range(n_heads)], axis=0)
    tall = n_heads * rows
    q_pos = lax.rem(lax.broadcasted_iota(jnp.int32, (tall, rows), 0), rows)
    k_pos = lax.broadcasted_iota(jnp.int32, (tall, rows), 1)
    own_scores = dot_nt(heads, near_kv[0:rows, 0:width])
    own_exp = jnp.where(jnp.abs(q_pos - k_pos) <= WINDOW, jnp.exp(own_scores), 0.0)
    with jax.named_scope("w_halo"):
        to_next.wait()
        to_last.wait()
    far_pos = jnp.where(k_pos < WINDOW, k_pos - WINDOW, k_pos + rows - WINDOW)
    low_pos = jnp.where(me == 0, 0, -WINDOW)
    high_pos = jnp.where(me == n_grid - 1, rows, rows + WINDOW)
    far_ok = (jnp.abs(q_pos - far_pos) <= WINDOW) & (far_pos >= low_pos) & (far_pos < high_pos)
    far_exp = jnp.where(far_ok, jnp.exp(dot_nt(heads, near_kv[rows:, 0:width])), 0.0)
    total = jnp.sum(own_exp, axis=-1, keepdims=True) + jnp.sum(far_exp, axis=-1, keepdims=True)
    mixed = dot((own_exp / total).astype(BF16), near_kv[0:rows, width:])
    mixed += dot((far_exp / total).astype(BF16), near_kv[rows:, width:])
    joined = mixed[0:rows]
    for h in range(1, n_heads):
        joined = jnp.where(head_lane == h, mixed[h * rows : (h + 1) * rows], joined)
    attended[band] = joined.astype(BF16)
    gather_start(ATT, attended.at[band])

    out_half = out_v.shape[2] // 2
    for k, q in enumerate(beside[: n_band // 2]):
        with jax.named_scope(f"w_out{q}"):
            x_wait(OUT, q, out_v.at[bands[q], mem])
        if n_band > 2:
            piece = out_v.at[bands[q], mem, pl.ds(k * out_half, out_half)]
            start(x_copy(PASS, n_band - q, piece, piece))
        start(mem_copy(OUT_OWN + q, out_v.at[bands[q], mem]))
    for q in near_bands:
        with jax.named_scope(f"w_dec{q}"):
            x_wait(DEC, q, dec_v.at[bands[q], mem])
        start(mem_copy(DEC_OWN + q, dec_v.at[bands[q], mem]))

    half_cols = out_v.shape[3]
    with jax.named_scope("w_outown"):
        mem_copy(OUT_OWN, out_v.at[band, other]).wait_recv()
    sums = [dot(attended[band], out_v[band, m]).astype(BF16).astype(F32) for m in range(2)]
    if n_band > 2:
        with jax.named_scope("w_pass"):
            for k, q in enumerate(beside):
                x_wait(PASS, q, out_v.at[bands[across], mem, pl.ds(k * out_half, out_half)])
        start(mem_copy(OUT_OWN + across, out_v.at[bands[across], mem]))

    with jax.named_scope("w_down"):
        mem_copy(DOWN, down_v.at[other]).wait_recv()
    for q in near_bands:
        with jax.named_scope(f"w_decmem{q}"):
            mem_copy(DEC_OWN + q, dec_v.at[bands[q], other]).wait_recv()
    fold = 0.0
    for k in range(n_band):
        per_half = half_cols // width
        columns = slice((k % per_half) * width, (k % per_half + 1) * width)
        fold += dot(down_v[k // per_half, :, columns], dec_v[k].reshape(width, -1))
    high, low = halves(fold)
    fold_v[0] = high
    fold_v[1] = low

    for q in near_bands:
        with jax.named_scope(f"w_att{q}"):
            x_wait(ATT, q, attended.at[bands[q]])
        with jax.named_scope(f"w_outmem{q}"):
            mem_copy(OUT_OWN + q, out_v.at[bands[q], other]).wait_recv()
        left = attended[bands[q]]
        for m in range(2):
            sums[m] = sums[m] + dot(left, out_v[bands[q], m]).astype(BF16).astype(F32)
    stream = stream_v[...] + jnp.concatenate(sums, axis=1)
    stream_v[...] = stream
    normed = rms_norm(stream).astype(BF16)

    with jax.named_scope("w_up"):
        mem_copy(UP, up_v.at[other]).wait_recv()
    deep = up_v.shape[1]
    hidden = gelu(dot(normed[:, :deep], up_v[0]) + dot(normed[:, deep:], up_v[1])).astype(BF16)
    high, low = halves(stream_v[:, pl.ds(pl.multiple_of(band * width, width), width)])
    own_dec = dec_v[band].reshape(width, -1)
    part = dot(hidden, fold_v[0]) + dot(hidden, fold_v[1]) + dot(high, own_dec) + dot(low, own_dec)
    proj[band] = part.astype(BF16)
    gather_start(PROJ, proj.at[band])
    z_sent(0, send_z, states)
    passed_on(states, STATES)
    for q in near_bands:
        with jax.named_scope(f"w_proj{q}"):
            x_wait(PROJ, q, proj.at[bands[q]])
        part = part + proj[bands[q]].astype(F32)
    nodes = part.astype(BF16)
    outgoing = dot_tn(select[0, 0:rows], nodes) + dot_tn(select[0, rows : 2 * rows], nodes)
    back_z[...] = outgoing.astype(BF16).reshape(back_z.shape)
    z_start(1, back_z, returned)
    for copy in sent:
        copy.wait_send()

    with jax.named_scope("w_back"):
        for p in range(per):
            z_wait(1, p, back_z, returned)
            pass_on(p, returned, BACKS)
    decoded = dot(pick[0], returned[0].reshape(group, -1))
    for q in near_bands:
        with jax.named_scope(f"w_xb{q}"):
            for k in range(2):
                x_wait(BACKS[k], q, returned.at[q, parts[k]])
        decoded += dot(pick[q], returned[q].reshape(group, -1))
    result = jnp.where(free_v[...] > 0.5, grid_v[...].astype(F32) + decoded, forcing_v[...].astype(F32))
    next_ref[...] = result.astype(BF16)
    z_sent(1, back_z, returned)
    passed_on(returned, BACKS)


def body(
    grid_state, forcing, boundary_mask, edge_src, edge_dst, edge_count, edge_weight,
    embed_weight, attn_qkv, attn_out, mlp_in, mlp_out, decode_weight,
):
    n_grid, n_band, n_mem = lax.axis_size("grid"), lax.axis_size("band"), lax.axis_size("mem")
    grid_rows = grid_state[0]
    points, channels = grid_rows.shape
    slots = edge_src.shape[2]
    model = decode_weight.shape[0] * n_band
    width = embed_weight.shape[1]
    rows = M_DEV
    per = n_grid // n_band
    group = per * slots
    operands = (
        grid_rows, forcing, boundary_mask.reshape(-1, channels), edge_src[0], edge_dst, edge_count.T, edge_weight, embed_weight,
        jnp.swapaxes(attn_qkv[0], 0, 1), attn_out[0], mlp_in[0], mlp_out[0], decode_weight,
    )
    vmem = pltpu.VMEM
    spread_over = {7: (n_band,), 8: (n_mem,), 9: (n_band, n_mem), 10: (n_mem,), 11: (n_mem,)}
    scratch = [vmem((*spread_over.get(k, ()), *a.shape), a.dtype) for k, a in enumerate(operands[:12])]
    scratch += [
        vmem((n_band, n_mem, width // n_mem, channels), BF16),
        vmem((n_band, points, group), BF16),
        vmem((n_band, 2 * rows, group), BF16),
        vmem((points, channels), F32),
        vmem((per, slots, channels), BF16),
        vmem((n_band, per, slots, channels), BF16),
        vmem((rows + 2 * WINDOW, 2 * width), BF16),
        vmem((n_band, rows, width), BF16),
        vmem((rows, model), F32),
        vmem((2, mlp_out.shape[1], channels), BF16),
        vmem((n_band, rows, channels), BF16),
        vmem((per, slots, channels), BF16),
        vmem((n_band, per, slots, channels), BF16),
        pltpu.SemaphoreType.DMA((14,)),
        pltpu.SemaphoreType.DMA((2, per)),
        pltpu.SemaphoreType.DMA((2, per)),
        pltpu.SemaphoreType.DMA((len(STAGES), n_band)),
        pltpu.SemaphoreType.DMA((len(STAGES), n_band)),
        pltpu.SemaphoreType.DMA((2 * n_band + 5,)),
        pltpu.SemaphoreType.DMA((2 * n_band + 5,)),
    ]
    result = pl.pallas_call(
        functools.partial(step_kernel, n_grid, n_band, model // HEADS),
        out_shape=jax.ShapeDtypeStruct((points, channels), BF16),
        in_specs=[pl.BlockSpec(memory_space=pl.ANY)] * len(operands),
        out_specs=pl.BlockSpec(memory_space=pltpu.VMEM),
        scratch_shapes=scratch,
        compiler_params=pltpu.CompilerParams(collective_id=0, has_side_effects=True),
    )(*operands)
    return result[None]


def solution(mesh):
    return jax.shard_map(
        body,
        mesh=mesh,
        in_specs=(
            P(("dom", "mem"), "grid", None),
            P(("dom", "grid"), None),
            P("grid"),
            P("grid", None, None),
            P(None, "grid", None),
            P(None, "grid"),
            P(None, "grid", None),
            P(None, "band"),
            P(None, "mem", None, "band"),
            P(None, "band", "mem"),
            P(None, "mem", "band"),
            P(None, "band", "mem"),
            P("band", None),
        ),
        out_specs=P(("dom", "mem"), "grid", None),
        check_vma=False,
    )
```

```python
import functools
import math

import jax
import jax.numpy as jnp
from jax import lax
from jax.experimental import pallas as pl
from jax.experimental.pallas import tpu as pltpu
from jax.sharding import PartitionSpec as P

HEADS = 16
M_DEV = 128
WINDOW = 64
EMBED, OUT, PASS, DEC, ATT, PROJ, *MORE = STAGES = range(10)
STATES, BACKS = MORE[:2], MORE[2:]
F32 = jnp.float32
BF16 = jnp.bfloat16
MESH = pl.DeviceIdType.MESH


def dot(left, right):
    return jnp.dot(left, right, preferred_element_type=F32)


def dot_tn(left, right):
    return lax.dot_general(left, right, (((0,), (0,)), ((), ())), preferred_element_type=F32)


def dot_nt(left, right):
    return lax.dot_general(left, right, (((1,), (1,)), ((), ())), preferred_element_type=F32)


def exact_dot(left, right):
    return jnp.dot(left, right, precision=lax.Precision.HIGHEST, preferred_element_type=F32)


def gelu(x):
    scale = math.sqrt(2.0 / math.pi)
    half = 0.5 * x
    return half * jnp.tanh(x * (x * x * (0.044715 * scale) + scale)) + half


def rms_norm(values):
    return values * lax.rsqrt(jnp.mean(values * values, axis=-1, keepdims=True) + 1e-06)


def halves(values):
    high = values.astype(BF16)
    return high, (values - high.astype(F32)).astype(BF16)


def step_kernel(
    n_grid, n_band, head_dim,
    grid_in, forcing_in, mask_in, src_in, dst_in, count_in, weight_in, embed_in, qkv_in, out_in, up_in, down_in, dec_in,
    next_ref,
    grid_v, forcing_v, mask_v, src_v, dst_v, count_v, weight_v, embed_v, qkv_v, out_v, up_v, down_v, dec_v,
    pick, select, free_v, send_z, relayed, states, near_kv, attended, stream_v, fold_v, proj, back_z, returned,
    load_sem, z_send, z_recv, hop_send, hop_recv, x_send, x_recv, mem_send, mem_recv,
):
    me = lax.axis_index("grid")
    band = lax.axis_index("band")
    mem = lax.axis_index("mem")
    other = 1 - mem
    per = n_grid // n_band
    slots = src_v.shape[1]
    group = per * slots
    up_next, down_next = lax.rem(me + 1, n_grid), lax.rem(me + n_grid - 1, n_grid)
    bands = [lax.rem(band + q, n_band) for q in range(n_band)]
    far_bands = sorted(range(1, n_band), key=lambda q: -min(q, n_band - q))
    near_bands = far_bands[::-1]
    beside, across = (1, n_band - 1), n_band // 2
    quarter, half_per = per // 4, per // 2
    order = [*range(quarter), *range(3 * quarter, per), *range(quarter, 3 * quarter)]
    ahead = [lax.rem(bands[q] + 2 * (n_grid - me), n_band) for q in range(n_band)]
    behind = [lax.rem(n_band - a, n_band) for a in ahead]
    is_self = ahead[0] == 0
    reach = n_grid // 4
    hops = (lax.rem(me + reach, n_grid), lax.rem(me + n_grid - reach, n_grid))

    def ahead_at(r):
        return lax.rem(me + ahead[0] + n_band * r, n_grid)

    def behind_at(r):
        return lax.rem(me + 2 * n_grid - behind[0] - n_band * r, n_grid)

    barrier = pltpu.get_barrier_semaphore()

    def greet(device):
        pl.semaphore_signal(barrier, inc=1, device_id=device, device_id_type=MESH)

    for p in range(half_per)[::-1]:
        if order[p] == 0:
            @pl.when(jnp.logical_not(is_self))
            def _():
                greet({"grid": ahead_at(0)})
        else:
            greet({"grid": ahead_at(order[p])})
    for device in hops:
        greet({"grid": device})
    greet({"grid": up_next})
    greet({"grid": down_next})
    for q in far_bands:
        greet({"band": bands[q]})
    greet({"mem": other})

    half = dec_v.shape[2]
    loads = [
        pltpu.make_async_copy(source, target, load_sem.at[k])
        for k, (source, target) in enumerate(
            (
                (src_in, src_v), (grid_in, grid_v), (embed_in, embed_v.at[band]),
                (dst_in, dst_v), (count_in, count_v), (weight_in, weight_v), (mask_in, mask_v), (forcing_in, forcing_v),
                (qkv_in, qkv_v.at[mem]), (out_in, out_v.at[band, mem]), (up_in, up_v.at[mem]), (down_in, down_v.at[mem]),
                (dec_in.at[0:half], dec_v.at[band, 0]), (dec_in.at[half : 2 * half], dec_v.at[band, 1]),
            )
        )
    ]
    for load in loads:
        load.start()

    span = half_per * slots
    lane = lax.broadcasted_iota(jnp.int32, (slots, span), 1)
    spread = jnp.where(lax.rem(lane, slots) == lax.broadcasted_iota(jnp.int32, (slots, span), 0), 1.0, 0.0).astype(F32)
    shard_row = lax.broadcasted_iota(jnp.int32, (n_grid, span), 0)
    place_lane = lax.broadcasted_iota(jnp.int32, (n_grid, span), 1) // slots
    step_lane = []
    for k in range(2):
        steps = jnp.zeros_like(place_lane)
        for p in range(half_per):
            steps = jnp.where(place_lane == p, n_band * order[k * half_per + p], steps)
        step_lane.append(steps)

    def lane_row(wide, shards):
        mine = shard_row == lax.rem(shards, n_grid)
        return jnp.sum(jnp.where(mine, wide, 0.0), axis=0, keepdims=True)

    point = lax.broadcasted_iota(jnp.int32, (grid_v.shape[0], span), 0).astype(F32)

    def build_pick(k, q):
        row = lane_row(src_wide, me + ahead[q] + step_lane[k])
        pick[k, :, q * span : (q + 1) * span] = jnp.where(point == row, 1.0, 0.0).astype(BF16)

    with jax.named_scope("w_load"):
        loads[0].wait()
        loads[1].wait()
    src_wide = exact_dot(src_v[...].astype(F32), spread)
    for k in range(2):
        build_pick(k, 0)
        send_z[k] = dot_tn(pick[k, :, 0:span], grid_v[...]).astype(BF16).reshape(send_z.shape[1:])

    with jax.named_scope("w_barrier"):
        pl.semaphore_wait(barrier, half_per + 4 + n_band - jnp.where(is_self, 1, 0))

    def at_place(ref, p):
        return ref.at[p // half_per, 0, p % half_per]

    def z_copy(way, p, source, target, device):
        return pltpu.make_async_remote_copy(
            src_ref=source, dst_ref=at_place(target, p), send_sem=z_send.at[way, p], recv_sem=z_recv.at[way, p],
            device_id={"grid": device}, device_id_type=MESH,
        )

    def z_own(way, p, source, target):
        return pltpu.make_async_copy(source, at_place(target, p), z_recv.at[way, p])

    def may_stay(way, p):
        return order[p] == 0 or (way == 0 and order[p] == quarter)

    def each_way(way, p, stay, go):
        if may_stay(way, p):
            if stay is not None:
                @pl.when(is_self)
                def _():
                    stay()

            @pl.when(jnp.logical_not(is_self))
            def _():
                go()
        else:
            go()

    def z_start(way, p, source, target, device):
        each_way(
            way, p, lambda: z_own(way, p, source, target).start(), lambda: z_copy(way, p, source, target, device).start()
        )

    def z_wait(way, p, target):
        here = at_place(target, p)
        each_way(
            way, p, lambda: z_own(way, p, here, target).wait(), lambda: z_copy(way, p, here, target, up_next).wait_recv()
        )

    def z_sent(way, target):
        for p in range(per):
            here = at_place(target, p)
            each_way(way, p, None, lambda: z_copy(way, p, here, target, up_next).wait_send())

    def hop_copy(k):
        return pltpu.make_async_remote_copy(
            src_ref=send_z.at[1, pl.ds(k * quarter, quarter)], dst_ref=relayed.at[k],
            send_sem=hop_send.at[k], recv_sem=hop_recv.at[k], device_id={"grid": hops[k]}, device_id_type=MESH,
        )

    def x_copy(stage, q, source, target):
        return pltpu.make_async_remote_copy(
            src_ref=source, dst_ref=target, send_sem=x_send.at[stage, q], recv_sem=x_recv.at[stage, n_band - q],
            device_id={"band": bands[q]}, device_id_type=MESH,
        )

    def x_wait(stage, q, target):
        pltpu.make_async_remote_copy(
            src_ref=target, dst_ref=target, send_sem=x_send.at[stage, q], recv_sem=x_recv.at[stage, q],
            device_id={"band": bands[q]}, device_id_type=MESH,
        ).wait_recv()

    def mem_copy(k, ref):
        return pltpu.make_async_remote_copy(
            src_ref=ref, dst_ref=ref, send_sem=mem_send.at[k], recv_sem=mem_recv.at[k],
            device_id={"mem": other}, device_id_type=MESH,
        )

    sent = []

    def start(copy):
        copy.start()
        sent.append(copy)

    def gather_start(stage, ref):
        for q in far_bands:
            start(x_copy(stage, q, ref, ref))

    QKV, UP, DOWN, OUT_OWN, DEC_OWN, LOW, HIGH = 0, 1, 2, 3, 3 + n_band, 3 + 2 * n_band, 4 + 2 * n_band

    for k in range(2):
        hop_copy(k).start()
    for p in range(half_per)[::-1]:
        z_start(0, p, send_z.at[0, p], states, ahead_at(order[p]))
    with jax.named_scope("w_load2"):
        loads[2].wait()
    gather_start(EMBED, embed_v.at[band])
    with jax.named_scope("w_load3"):
        for load in loads[3:]:
            load.wait()
    for k, ref in ((QKV, qkv_v), (DOWN, down_v), (UP, up_v)):
        start(mem_copy(k, ref.at[mem]))
    start(mem_copy(OUT_OWN, out_v.at[band, mem]))
    for q in far_bands:
        start(x_copy(DEC, q, dec_v.at[band, mem], dec_v.at[band, mem]))
    for q in beside[: n_band // 2]:
        start(x_copy(OUT, q, out_v.at[band, mem], out_v.at[band, mem]))

    rows = stream_v.shape[0]
    square_row = lax.broadcasted_iota(jnp.int32, (n_grid, n_grid), 0)
    square_lane = lax.broadcasted_iota(jnp.int32, (n_grid, n_grid), 1)
    counts = jnp.sum(jnp.where(square_row == square_lane, count_v[...].astype(F32), 0.0), axis=1, keepdims=True)
    slot_lane = lax.broadcasted_iota(jnp.int32, (n_grid, slots), 1).astype(F32)
    live = jnp.where(slot_lane < counts, weight_v[:, 0, :], 0.0)
    dst_wide = exact_dot(dst_v[:, 0, :].astype(F32), spread)
    live_wide = exact_dot(live, spread)
    node = lax.broadcasted_iota(jnp.int32, (rows, span), 0).astype(F32)

    def build_tables(k):
        for q in range(n_band):
            shards = me + 2 * n_grid - behind[q] - step_lane[k]
            table = jnp.where(node == lane_row(dst_wide, shards), lane_row(live_wide, shards), 0.0)
            high, low = halves(table)
            select[k, 0:rows, q * span : (q + 1) * span] = high
            select[k, rows : 2 * rows, q * span : (q + 1) * span] = low
            if q:
                build_pick(k, q)

    build_tables(0)
    build_tables(1)
    lanes = mask_v.shape[1]
    diagonal = lax.broadcasted_iota(jnp.int32, (lanes, lanes), 0) == lax.broadcasted_iota(jnp.int32, (lanes, lanes), 1)
    for k in range(mask_v.shape[0]):
        flags = jnp.where(mask_v[k : k + 1, :] == 1, 0.0, 1.0).astype(F32)
        column = jnp.sum(jnp.where(diagonal, flags, 0.0), axis=1, keepdims=True)
        free_v[k * lanes : (k + 1) * lanes] = jnp.broadcast_to(column, (lanes, free_v.shape[1]))

    with jax.named_scope("w_hop"):
        for k in range(2):
            hop_copy(k).wait_recv()
            for t in range(quarter):
                z_start(0, half_per + k * quarter + t, relayed.at[k, t], states, ahead_at((0, 3 * quarter)[k] + t))

    def pass_on(p, ref, stages):
        k, t = p // half_per, p % half_per
        for q in far_bands:
            x_copy(stages[k], q, ref.at[k, 0, t], ref.at[k, n_band - q, t]).start()

    def passed_on(ref, stages):
        for k in range(2):
            for q in far_bands:
                x_copy(stages[k], q, ref.at[k, 0], ref.at[k, n_band - q]).wait_send()

    width = embed_v.shape[2]

    def encode(block, table, first=False):
        for col in range(n_band):
            both = dot(table, gelu(dot(block, embed_v[col])).astype(BF16))
            part = both[:rows] + both[rows:]
            cols = slice(col * width, (col + 1) * width)
            stream_v[:, cols] = part if first else stream_v[:, cols] + part

    with jax.named_scope("w_znear"):
        for p in range(half_per):
            z_wait(0, p, states)
            pass_on(p, states, STATES)
    with jax.named_scope("w_zfar"):
        for p in range(half_per, per):
            z_wait(0, p, states)
            pass_on(p, states, STATES)
    out_half = out_v.shape[2] // 2
    with jax.named_scope("w_dec"):
        for q in near_bands:
            x_wait(DEC, q, dec_v.at[bands[q], mem])
            start(mem_copy(DEC_OWN + q, dec_v.at[bands[q], mem]))
    with jax.named_scope("w_out"):
        for k, q in enumerate(beside[: n_band // 2]):
            x_wait(OUT, q, out_v.at[bands[q], mem])
            if n_band > 2:
                piece = out_v.at[bands[q], mem, pl.ds(k * out_half, out_half)]
                start(x_copy(PASS, n_band - q, piece, piece))
            start(mem_copy(OUT_OWN + q, out_v.at[bands[q], mem]))
    with jax.named_scope("w_embed"):
        for q in near_bands:
            x_wait(EMBED, q, embed_v.at[bands[q]])
    own = jnp.concatenate([states[k, 0].reshape(span, -1) for k in range(2)], axis=0)
    encode(own, jnp.concatenate([select[k, :, 0:span] for k in range(2)], axis=1), True)
    with jax.named_scope("w_xnear"):
        for q in near_bands:
            x_wait(STATES[0], q, states.at[0, q])
    encode(states[0, 1:].reshape((n_band - 1) * span, -1), select[0, :, span:])

    half_cols = out_v.shape[3]
    with jax.named_scope("w_down"):
        mem_copy(DOWN, down_v.at[other]).wait_recv()
        for q in near_bands:
            mem_copy(DEC_OWN + q, dec_v.at[bands[q], other]).wait_recv()
    fold = 0.0
    for k in range(n_band):
        per_half = half_cols // width
        columns = slice((k % per_half) * width, (k % per_half + 1) * width)
        fold += dot(down_v[k // per_half, :, columns], dec_v[k].reshape(width, -1))
    high, low = halves(fold)
    fold_v[0] = high
    fold_v[1] = low

    with jax.named_scope("w_xfar"):
        for q in near_bands:
            x_wait(STATES[1], q, states.at[1, q])
    encode(states[1, 1:].reshape((n_band - 1) * span, -1), select[1, :, span:])
    stream = stream_v[...].astype(BF16).astype(F32)
    stream_v[...] = stream
    normed = rms_norm(stream).astype(BF16)

    with jax.named_scope("w_qkv"):
        mem_copy(QKV, qkv_v.at[other]).wait_recv()
    deep = qkv_v.shape[2]

    def project(which):
        return dot(normed[:, :deep], qkv_v[0, which]) + dot(normed[:, deep:], qkv_v[1, which])

    lane_r = lax.broadcasted_iota(jnp.int32, (width, width), 0) // head_dim
    lane_c = lax.broadcasted_iota(jnp.int32, (width, width), 1) // head_dim
    head_mean = jnp.where(lane_r == lane_c, 1.0 / head_dim, 0.0).astype(BF16)

    def head_norm(values):
        high, low = halves(values * values)
        return values * lax.rsqrt(dot(high, head_mean) + dot(low, head_mean) + 1e-06)

    near_kv[0:rows, 0:width] = head_norm(project(1)).astype(BF16)
    near_kv[0:rows, width:] = project(2).astype(BF16)
    lower, upper = pl.ds(rows, WINDOW), pl.ds(rows + WINDOW, WINDOW)

    def halo(k, source, target, device):
        return pltpu.make_async_remote_copy(
            src_ref=near_kv.at[source], dst_ref=near_kv.at[target], send_sem=mem_send.at[k], recv_sem=mem_recv.at[k],
            device_id={"grid": device}, device_id_type=MESH,
        )

    to_next = halo(LOW, pl.ds(rows - WINDOW, WINDOW), lower, up_next)
    to_last = halo(HIGH, pl.ds(0, WINDOW), upper, down_next)
    to_next.start()
    to_last.start()

    n_heads = width // head_dim
    query = head_norm(project(0)).astype(BF16) * jnp.asarray(head_dim**-0.5, BF16)
    head_lane = lax.broadcasted_iota(jnp.int32, (rows, width), 1) // head_dim
    zero = jnp.zeros_like(query)
    heads = jnp.concatenate([jnp.where(head_lane == h, query, zero) for h in range(n_heads)], axis=0)
    tall = n_heads * rows
    q_pos = lax.rem(lax.broadcasted_iota(jnp.int32, (tall, rows), 0), rows)
    k_pos = lax.broadcasted_iota(jnp.int32, (tall, rows), 1)
    own_scores = dot_nt(heads, near_kv[0:rows, 0:width])
    own_exp = jnp.where(jnp.abs(q_pos - k_pos) <= WINDOW, jnp.exp(own_scores), 0.0)
    if n_band > 2:
        with jax.named_scope("w_pass"):
            for k, q in enumerate(beside):
                x_wait(PASS, q, out_v.at[bands[across], mem, pl.ds(k * out_half, out_half)])
        start(mem_copy(OUT_OWN + across, out_v.at[bands[across], mem]))
    with jax.named_scope("w_halo"):
        to_next.wait()
        to_last.wait()
    far_pos = jnp.where(k_pos < WINDOW, k_pos - WINDOW, k_pos + rows - WINDOW)
    low_pos = jnp.where(me == 0, 0, -WINDOW)
    high_pos = jnp.where(me == n_grid - 1, rows, rows + WINDOW)
    far_ok = (jnp.abs(q_pos - far_pos) <= WINDOW) & (far_pos >= low_pos) & (far_pos < high_pos)
    far_exp = jnp.where(far_ok, jnp.exp(dot_nt(heads, near_kv[rows:, 0:width])), 0.0)
    total = jnp.sum(own_exp, axis=-1, keepdims=True) + jnp.sum(far_exp, axis=-1, keepdims=True)
    mixed = dot((own_exp / total).astype(BF16), near_kv[0:rows, width:])
    mixed += dot((far_exp / total).astype(BF16), near_kv[rows:, width:])
    joined = mixed[0:rows]
    for h in range(1, n_heads):
        joined = jnp.where(head_lane == h, mixed[h * rows : (h + 1) * rows], joined)
    attended[band] = joined.astype(BF16)
    gather_start(ATT, attended.at[band])

    with jax.named_scope("w_outown"):
        mem_copy(OUT_OWN, out_v.at[band, other]).wait_recv()
    sums = [dot(attended[band], out_v[band, m]).astype(BF16).astype(F32) for m in range(2)]
    for q in near_bands:
        with jax.named_scope(f"w_att{q}"):
            x_wait(ATT, q, attended.at[bands[q]])
        with jax.named_scope(f"w_outmem{q}"):
            mem_copy(OUT_OWN + q, out_v.at[bands[q], other]).wait_recv()
        left = attended[bands[q]]
        for m in range(2):
            sums[m] = sums[m] + dot(left, out_v[bands[q], m]).astype(BF16).astype(F32)
    stream = stream_v[...] + jnp.concatenate(sums, axis=1)
    stream_v[...] = stream
    normed = rms_norm(stream).astype(BF16)

    with jax.named_scope("w_up"):
        mem_copy(UP, up_v.at[other]).wait_recv()
    deep = up_v.shape[1]
    hidden = gelu(dot(normed[:, :deep], up_v[0]) + dot(normed[:, deep:], up_v[1])).astype(BF16)
    high, low = halves(stream_v[:, pl.ds(pl.multiple_of(band * width, width), width)])
    own_dec = dec_v[band].reshape(width, -1)
    part = dot(hidden, fold_v[0]) + dot(hidden, fold_v[1]) + dot(high, own_dec) + dot(low, own_dec)
    proj[band] = part.astype(BF16)
    gather_start(PROJ, proj.at[band])
    z_sent(0, states)
    for k in range(2):
        hop_copy(k).wait_send()
    passed_on(states, STATES)
    for q in near_bands:
        with jax.named_scope(f"w_proj{q}"):
            x_wait(PROJ, q, proj.at[bands[q]])
        part = part + proj[bands[q]].astype(F32)
    nodes = part.astype(BF16)
    for k in (1, 0):
        outgoing = dot_tn(select[k, 0:rows, 0:span], nodes) + dot_tn(select[k, rows : 2 * rows, 0:span], nodes)
        back_z[k] = outgoing.astype(BF16).reshape(back_z.shape[1:])
        for t in range(half_per):
            p = k * half_per + t
            z_start(1, p, back_z.at[k, t], returned, behind_at(order[p]))
    for copy in sent:
        copy.wait_send()

    with jax.named_scope("w_back"):
        for p in range(per):
            z_wait(1, p, returned)
            pass_on(p, returned, BACKS)
    decoded = 0.0
    for k in range(2):
        decoded += dot(pick[k, :, 0:span], returned[k, 0].reshape(span, -1))
    for k in range(2):
        with jax.named_scope(f"w_xb{k}"):
            for q in near_bands:
                x_wait(BACKS[k], q, returned.at[k, q])
        decoded += dot(pick[k, :, span:], returned[k, 1:].reshape((n_band - 1) * span, -1))
    result = jnp.where(free_v[...] > 0.5, grid_v[...].astype(F32) + decoded, forcing_v[...].astype(F32))
    next_ref[...] = result.astype(BF16)
    z_sent(1, returned)
    passed_on(returned, BACKS)


def body(
    grid_state, forcing, boundary_mask, edge_src, edge_dst, edge_count, edge_weight,
    embed_weight, attn_qkv, attn_out, mlp_in, mlp_out, decode_weight,
):
    n_grid, n_band, n_mem = lax.axis_size("grid"), lax.axis_size("band"), lax.axis_size("mem")
    grid_rows = grid_state[0]
    points, channels = grid_rows.shape
    slots = edge_src.shape[2]
    model = decode_weight.shape[0] * n_band
    width = embed_weight.shape[1]
    rows = M_DEV
    per = n_grid // n_band
    group = per * slots
    operands = (
        grid_rows, forcing, boundary_mask.reshape(-1, channels), edge_src[0], edge_dst, edge_count.T, edge_weight, embed_weight,
        jnp.swapaxes(attn_qkv[0], 0, 1), attn_out[0], mlp_in[0], mlp_out[0], decode_weight,
    )
    vmem = pltpu.VMEM
    spread_over = {7: (n_band,), 8: (n_mem,), 9: (n_band, n_mem), 10: (n_mem,), 11: (n_mem,)}
    scratch = [vmem((*spread_over.get(k, ()), *a.shape), a.dtype) for k, a in enumerate(operands[:12])]
    scratch += [
        vmem((n_band, n_mem, width // n_mem, channels), BF16),
        vmem((2, points, n_band * group // 2), BF16),
        vmem((2, 2 * rows, n_band * group // 2), BF16),
        vmem((points, channels), F32),
        vmem((2, per // 2, slots, channels), BF16),
        vmem((2, per // 4, slots, channels), BF16),
        vmem((2, n_band, per // 2, slots, channels), BF16),
        vmem((rows + 2 * WINDOW, 2 * width), BF16),
        vmem((n_band, rows, width), BF16),
        vmem((rows, model), F32),
        vmem((2, mlp_out.shape[1], channels), BF16),
        vmem((n_band, rows, channels), BF16),
        vmem((2, per // 2, slots, channels), BF16),
        vmem((2, n_band, per // 2, slots, channels), BF16),
        pltpu.SemaphoreType.DMA((14,)),
        pltpu.SemaphoreType.DMA((2, per)),
        pltpu.SemaphoreType.DMA((2, per)),
        pltpu.SemaphoreType.DMA((2,)),
        pltpu.SemaphoreType.DMA((2,)),
        pltpu.SemaphoreType.DMA((len(STAGES), n_band)),
        pltpu.SemaphoreType.DMA((len(STAGES), n_band)),
        pltpu.SemaphoreType.DMA((2 * n_band + 5,)),
        pltpu.SemaphoreType.DMA((2 * n_band + 5,)),
    ]
    result = pl.pallas_call(
        functools.partial(step_kernel, n_grid, n_band, model // HEADS),
        out_shape=jax.ShapeDtypeStruct((points, channels), BF16),
        in_specs=[pl.BlockSpec(memory_space=pl.ANY)] * len(operands),
        out_specs=pl.BlockSpec(memory_space=pltpu.VMEM),
        scratch_shapes=scratch,
        compiler_params=pltpu.CompilerParams(collective_id=0, has_side_effects=True),
    )(*operands)
    return result[None]


def solution(mesh):
    return jax.shard_map(
        body,
        mesh=mesh,
        in_specs=(
            P(("dom", "mem"), "grid", None),
            P(("dom", "grid"), None),
            P("grid"),
            P("grid", None, None),
            P(None, "grid", None),
            P(None, "grid"),
            P(None, "grid", None),
            P(None, "band"),
            P(None, "mem", None, "band"),
            P(None, "band", "mem"),
            P(None, "mem", "band"),
            P(None, "band", "mem"),
            P("band", None),
        ),
        out_specs=P(("dom", "mem"), "grid", None),
        check_vma=False,
    )
```

```python
import functools
import math

import jax
import jax.numpy as jnp
from jax import lax
from jax.experimental import pallas as pl
from jax.experimental.pallas import tpu as pltpu
from jax.sharding import PartitionSpec as P

HEADS = 16
M_DEV = 128
WINDOW = 64
VMEM_BYTES = 61_500_000
EMBED, OUT, PASS, DEC, ATT, PROJ, *MORE = STAGES = range(10)
STATES, BACKS = MORE[:2], MORE[2:]
F32 = jnp.float32
BF16 = jnp.bfloat16
MESH = pl.DeviceIdType.MESH


def dot(left, right):
    return jnp.dot(left, right, preferred_element_type=F32)


def dot_tn(left, right):
    return lax.dot_general(left, right, (((0,), (0,)), ((), ())), preferred_element_type=F32)


def dot_nt(left, right):
    return lax.dot_general(left, right, (((1,), (1,)), ((), ())), preferred_element_type=F32)


def exact_dot(left, right):
    return jnp.dot(left, right, precision=lax.Precision.HIGHEST, preferred_element_type=F32)


def gelu(x):
    scale = math.sqrt(2.0 / math.pi)
    half = 0.5 * x
    return half * jnp.tanh(x * (x * x * (0.044715 * scale) + scale)) + half


def rms_norm(values):
    return values * lax.rsqrt(jnp.mean(values * values, axis=-1, keepdims=True) + 1e-06)


def halves(values):
    high = values.astype(BF16)
    return high, (values - high.astype(F32)).astype(BF16)


def step_kernel(
    n_grid, n_band, head_dim,
    grid_in, forcing_in, mask_in, src_in, dst_in, count_in, weight_in, embed_in, qkv_in, out_in, up_in, down_in, dec_in,
    next_ref,
    grid_v, forcing_v, mask_v, src_v, dst_v, count_v, weight_v, embed_v, qkv_v, out_v, up_v, down_v, dec_v,
    pick, select, free_v, send_z, relayed, states, near_kv, attended, stream_v, fold_v, proj, back_z, returned,
    load_sem, z_send, z_recv, hop_send, hop_recv, x_send, x_recv, mem_send, mem_recv,
):
    me = lax.axis_index("grid")
    band = lax.axis_index("band")
    mem = lax.axis_index("mem")
    other = 1 - mem
    per = n_grid // n_band
    slots = src_v.shape[1]
    group = per * slots
    up_next, down_next = lax.rem(me + 1, n_grid), lax.rem(me + n_grid - 1, n_grid)
    bands = [lax.rem(band + q, n_band) for q in range(n_band)]
    far_bands = sorted(range(1, n_band), key=lambda q: -min(q, n_band - q))
    near_bands = far_bands[::-1]
    beside, across = (1, n_band - 1), n_band // 2
    quarter, half_per = per // 4, per // 2
    order = [*range(quarter), *range(3 * quarter, per), *range(quarter, 3 * quarter)]
    ahead = [lax.rem(bands[q] + 2 * (n_grid - me), n_band) for q in range(n_band)]
    behind = [lax.rem(n_band - a, n_band) for a in ahead]
    is_self = ahead[0] == 0
    reach = n_grid // 4
    hops = (lax.rem(me + reach, n_grid), lax.rem(me + n_grid - reach, n_grid))

    def ahead_at(r):
        return lax.rem(me + ahead[0] + n_band * r, n_grid)

    def behind_at(r):
        return lax.rem(me + 2 * n_grid - behind[0] - n_band * r, n_grid)

    half = dec_v.shape[2]
    loads = [
        pltpu.make_async_copy(source, target, load_sem.at[k])
        for k, (source, target) in enumerate(
            (
                (src_in, src_v), (grid_in, grid_v), (embed_in, embed_v.at[band]),
                (dst_in, dst_v), (count_in, count_v), (weight_in, weight_v), (mask_in, mask_v), (forcing_in, forcing_v),
                (qkv_in, qkv_v.at[mem]), (out_in, out_v.at[band, mem]), (up_in, up_v.at[mem]), (down_in, down_v.at[mem]),
                (dec_in.at[0:half], dec_v.at[band, 0]), (dec_in.at[half : 2 * half], dec_v.at[band, 1]),
            )
        )
    ]
    loads[0].start()
    loads[1].start()

    barrier = pltpu.get_barrier_semaphore()

    def greet(device):
        pl.semaphore_signal(barrier, inc=1, device_id=device, device_id_type=MESH)

    for p in range(half_per)[::-1]:
        if order[p] == 0:
            @pl.when(jnp.logical_not(is_self))
            def _():
                greet({"grid": ahead_at(0)})
        else:
            greet({"grid": ahead_at(order[p])})
    for device in hops:
        greet({"grid": device})
    greet({"grid": up_next})
    greet({"grid": down_next})
    for q in far_bands:
        greet({"band": bands[q]})
    greet({"mem": other})

    for load in loads[2:]:
        load.start()

    span = half_per * slots
    lane = lax.broadcasted_iota(jnp.int32, (slots, span), 1)
    spread = jnp.where(lax.rem(lane, slots) == lax.broadcasted_iota(jnp.int32, (slots, span), 0), 1.0, 0.0).astype(F32)
    shard_row = lax.broadcasted_iota(jnp.int32, (n_grid, span), 0)
    place_lane = lax.broadcasted_iota(jnp.int32, (n_grid, span), 1) // slots
    step_lane = []
    for k in range(2):
        steps = jnp.zeros_like(place_lane)
        for p in range(half_per):
            steps = jnp.where(place_lane == p, n_band * order[k * half_per + p], steps)
        step_lane.append(steps)

    def lane_row(wide, shards):
        mine = shard_row == lax.rem(shards, n_grid)
        return jnp.sum(jnp.where(mine, wide, 0.0), axis=0, keepdims=True)

    point = lax.broadcasted_iota(jnp.int32, (grid_v.shape[0], span), 0).astype(F32)

    def build_pick(k, q):
        row = lane_row(src_wide, me + ahead[q] + step_lane[k])
        pick[k, :, q * span : (q + 1) * span] = jnp.where(point == row, 1.0, 0.0).astype(BF16)

    with jax.named_scope("w_load"):
        loads[0].wait()
        loads[1].wait()
    src_wide = exact_dot(src_v[...].astype(F32), spread)
    for k in range(2):
        build_pick(k, 0)
        send_z[k] = dot_tn(pick[k, :, 0:span], grid_v[...]).astype(BF16).reshape(send_z.shape[1:])

    with jax.named_scope("w_barrier"):
        pl.semaphore_wait(barrier, half_per + 4 + n_band - jnp.where(is_self, 1, 0))

    def at_place(ref, p):
        return ref.at[p // half_per, 0, p % half_per]

    def z_copy(way, p, source, target, device):
        return pltpu.make_async_remote_copy(
            src_ref=source, dst_ref=at_place(target, p), send_sem=z_send.at[way, p], recv_sem=z_recv.at[way, p],
            device_id={"grid": device}, device_id_type=MESH,
        )

    def z_own(way, p, source, target):
        return pltpu.make_async_copy(source, at_place(target, p), z_recv.at[way, p])

    def may_stay(way, p):
        return order[p] == 0 or (way == 0 and order[p] == quarter)

    def each_way(way, p, stay, go):
        if may_stay(way, p):
            if stay is not None:
                @pl.when(is_self)
                def _():
                    stay()

            @pl.when(jnp.logical_not(is_self))
            def _():
                go()
        else:
            go()

    def z_start(way, p, source, target, device):
        each_way(
            way, p, lambda: z_own(way, p, source, target).start(), lambda: z_copy(way, p, source, target, device).start()
        )

    def z_wait(way, p, target):
        here = at_place(target, p)
        each_way(
            way, p, lambda: z_own(way, p, here, target).wait(), lambda: z_copy(way, p, here, target, up_next).wait_recv()
        )

    def z_sent(way, target):
        for p in range(per):
            here = at_place(target, p)
            each_way(way, p, None, lambda: z_copy(way, p, here, target, up_next).wait_send())

    def hop_copy(k):
        return pltpu.make_async_remote_copy(
            src_ref=send_z.at[1, pl.ds(k * quarter, quarter)], dst_ref=relayed.at[k],
            send_sem=hop_send.at[k], recv_sem=hop_recv.at[k], device_id={"grid": hops[k]}, device_id_type=MESH,
        )

    def x_copy(stage, q, source, target):
        return pltpu.make_async_remote_copy(
            src_ref=source, dst_ref=target, send_sem=x_send.at[stage, q], recv_sem=x_recv.at[stage, n_band - q],
            device_id={"band": bands[q]}, device_id_type=MESH,
        )

    def x_wait(stage, q, target):
        pltpu.make_async_remote_copy(
            src_ref=target, dst_ref=target, send_sem=x_send.at[stage, q], recv_sem=x_recv.at[stage, q],
            device_id={"band": bands[q]}, device_id_type=MESH,
        ).wait_recv()

    def mem_copy(k, ref):
        return pltpu.make_async_remote_copy(
            src_ref=ref, dst_ref=ref, send_sem=mem_send.at[k], recv_sem=mem_recv.at[k],
            device_id={"mem": other}, device_id_type=MESH,
        )

    sent = []

    def start(copy):
        copy.start()
        sent.append(copy)

    def gather_start(stage, ref):
        for q in far_bands:
            start(x_copy(stage, q, ref, ref))

    QKV, UP, DOWN, OUT_OWN, DEC_OWN, LOW, HIGH = 0, 1, 2, 3, 3 + n_band, 3 + 2 * n_band, 4 + 2 * n_band

    for k in range(2):
        hop_copy(k).start()
    for p in range(half_per)[::-1]:
        z_start(0, p, send_z.at[0, p], states, ahead_at(order[p]))
    with jax.named_scope("w_load2"):
        loads[2].wait()
    gather_start(EMBED, embed_v.at[band])
    with jax.named_scope("w_load3"):
        for load in loads[3:]:
            load.wait()
    for k, ref in ((QKV, qkv_v), (DOWN, down_v), (UP, up_v)):
        start(mem_copy(k, ref.at[mem]))
    start(mem_copy(OUT_OWN, out_v.at[band, mem]))
    for q in far_bands:
        start(x_copy(DEC, q, dec_v.at[band, mem], dec_v.at[band, mem]))
    for q in beside[: n_band // 2]:
        start(x_copy(OUT, q, out_v.at[band, mem], out_v.at[band, mem]))

    rows = stream_v.shape[0]
    square_row = lax.broadcasted_iota(jnp.int32, (n_grid, n_grid), 0)
    square_lane = lax.broadcasted_iota(jnp.int32, (n_grid, n_grid), 1)
    counts = jnp.sum(jnp.where(square_row == square_lane, count_v[...].astype(F32), 0.0), axis=1, keepdims=True)
    slot_lane = lax.broadcasted_iota(jnp.int32, (n_grid, slots), 1).astype(F32)
    live = jnp.where(slot_lane < counts, weight_v[:, 0, :], 0.0)
    dst_wide = exact_dot(dst_v[:, 0, :].astype(F32), spread)
    live_wide = exact_dot(live, spread)
    node = lax.broadcasted_iota(jnp.int32, (rows, span), 0).astype(F32)

    def build_tables(k):
        for q in range(n_band):
            shards = me + 2 * n_grid - behind[q] - step_lane[k]
            table = jnp.where(node == lane_row(dst_wide, shards), lane_row(live_wide, shards), 0.0)
            high, low = halves(table)
            select[k, 0:rows, q * span : (q + 1) * span] = high
            select[k, rows : 2 * rows, q * span : (q + 1) * span] = low
            if q:
                build_pick(k, q)

    build_tables(0)
    build_tables(1)
    lanes = mask_v.shape[1]
    diagonal = lax.broadcasted_iota(jnp.int32, (lanes, lanes), 0) == lax.broadcasted_iota(jnp.int32, (lanes, lanes), 1)
    for k in range(mask_v.shape[0]):
        flags = jnp.where(mask_v[k : k + 1, :] == 1, 0.0, 1.0).astype(F32)
        column = jnp.sum(jnp.where(diagonal, flags, 0.0), axis=1, keepdims=True)
        free_v[k * lanes : (k + 1) * lanes] = jnp.broadcast_to(column, (lanes, free_v.shape[1]))

    with jax.named_scope("w_hop"):
        for k in range(2):
            hop_copy(k).wait_recv()
            for t in range(quarter):
                z_start(0, half_per + k * quarter + t, relayed.at[k, t], states, ahead_at((0, 3 * quarter)[k] + t))

    def pass_on(p, ref, stages):
        k, t = p // half_per, p % half_per
        for q in far_bands:
            x_copy(stages[k], q, ref.at[k, 0, t], ref.at[k, n_band - q, t]).start()

    def passed_on(ref, stages):
        for k in range(2):
            for q in far_bands:
                x_copy(stages[k], q, ref.at[k, 0], ref.at[k, n_band - q]).wait_send()

    width = embed_v.shape[2]

    def encode(block, table, first=False):
        for col in range(n_band):
            both = dot(table, gelu(dot(block, embed_v[col])).astype(BF16))
            part = both[:rows] + both[rows:]
            cols = slice(col * width, (col + 1) * width)
            stream_v[:, cols] = part if first else stream_v[:, cols] + part

    with jax.named_scope("w_znear"):
        for p in range(half_per):
            z_wait(0, p, states)
            pass_on(p, states, STATES)
    with jax.named_scope("w_zfar"):
        for p in range(half_per, per):
            z_wait(0, p, states)
            pass_on(p, states, STATES)
    out_half = out_v.shape[2] // 2
    with jax.named_scope("w_dec"):
        for q in near_bands:
            x_wait(DEC, q, dec_v.at[bands[q], mem])
            start(mem_copy(DEC_OWN + q, dec_v.at[bands[q], mem]))
    with jax.named_scope("w_out"):
        for k, q in enumerate(beside[: n_band // 2]):
            x_wait(OUT, q, out_v.at[bands[q], mem])
            if n_band > 2:
                piece = out_v.at[bands[q], mem, pl.ds(k * out_half, out_half)]
                start(x_copy(PASS, n_band - q, piece, piece))
            start(mem_copy(OUT_OWN + q, out_v.at[bands[q], mem]))
    with jax.named_scope("w_embed"):
        for q in near_bands:
            x_wait(EMBED, q, embed_v.at[bands[q]])
    own = jnp.concatenate([states[k, 0].reshape(span, -1) for k in range(2)], axis=0)
    encode(own, jnp.concatenate([select[k, :, 0:span] for k in range(2)], axis=1), True)
    with jax.named_scope("w_xnear"):
        for q in near_bands:
            x_wait(STATES[0], q, states.at[0, q])
    encode(states[0, 1:].reshape((n_band - 1) * span, -1), select[0, :, span:])

    half_cols = out_v.shape[3]
    with jax.named_scope("w_down"):
        mem_copy(DOWN, down_v.at[other]).wait_recv()
        for q in near_bands:
            mem_copy(DEC_OWN + q, dec_v.at[bands[q], other]).wait_recv()
    fold = 0.0
    for k in range(n_band):
        per_half = half_cols // width
        columns = slice((k % per_half) * width, (k % per_half + 1) * width)
        fold += dot(down_v[k // per_half, :, columns], dec_v[k].reshape(width, -1))
    high, low = halves(fold)
    fold_v[0] = high
    fold_v[1] = low

    with jax.named_scope("w_xfar"):
        for q in near_bands:
            x_wait(STATES[1], q, states.at[1, q])
    encode(states[1, 1:].reshape((n_band - 1) * span, -1), select[1, :, span:])
    stream = stream_v[...].astype(BF16).astype(F32)
    stream_v[...] = stream
    normed = rms_norm(stream).astype(BF16)

    with jax.named_scope("w_qkv"):
        mem_copy(QKV, qkv_v.at[other]).wait_recv()
    deep = qkv_v.shape[2]

    def project(which):
        return dot(normed[:, :deep], qkv_v[0, which]) + dot(normed[:, deep:], qkv_v[1, which])

    lane_r = lax.broadcasted_iota(jnp.int32, (width, width), 0) // head_dim
    lane_c = lax.broadcasted_iota(jnp.int32, (width, width), 1) // head_dim
    head_mean = jnp.where(lane_r == lane_c, 1.0 / head_dim, 0.0).astype(BF16)

    def head_norm(values):
        high, low = halves(values * values)
        return values * lax.rsqrt(dot(high, head_mean) + dot(low, head_mean) + 1e-06)

    near_kv[0:rows, 0:width] = head_norm(project(1)).astype(BF16)
    near_kv[0:rows, width:] = project(2).astype(BF16)
    lower, upper = pl.ds(rows, WINDOW), pl.ds(rows + WINDOW, WINDOW)

    def halo(k, source, target, device):
        return pltpu.make_async_remote_copy(
            src_ref=near_kv.at[source], dst_ref=near_kv.at[target], send_sem=mem_send.at[k], recv_sem=mem_recv.at[k],
            device_id={"grid": device}, device_id_type=MESH,
        )

    to_next = halo(LOW, pl.ds(rows - WINDOW, WINDOW), lower, up_next)
    to_last = halo(HIGH, pl.ds(0, WINDOW), upper, down_next)
    to_next.start()
    to_last.start()

    n_heads = width // head_dim
    query = head_norm(project(0)).astype(BF16) * jnp.asarray(head_dim**-0.5, BF16)
    head_lane = lax.broadcasted_iota(jnp.int32, (rows, width), 1) // head_dim
    zero = jnp.zeros_like(query)
    heads = jnp.concatenate([jnp.where(head_lane == h, query, zero) for h in range(n_heads)], axis=0)
    tall = n_heads * rows
    q_pos = lax.rem(lax.broadcasted_iota(jnp.int32, (tall, rows), 0), rows)
    k_pos = lax.broadcasted_iota(jnp.int32, (tall, rows), 1)
    own_scores = dot_nt(heads, near_kv[0:rows, 0:width])
    own_exp = jnp.where(jnp.abs(q_pos - k_pos) <= WINDOW, jnp.exp(own_scores), 0.0)
    if n_band > 2:
        with jax.named_scope("w_pass"):
            for k, q in enumerate(beside):
                x_wait(PASS, q, out_v.at[bands[across], mem, pl.ds(k * out_half, out_half)])
        start(mem_copy(OUT_OWN + across, out_v.at[bands[across], mem]))
    with jax.named_scope("w_halo"):
        to_next.wait()
        to_last.wait()
    far_pos = jnp.where(k_pos < WINDOW, k_pos - WINDOW, k_pos + rows - WINDOW)
    low_pos = jnp.where(me == 0, 0, -WINDOW)
    high_pos = jnp.where(me == n_grid - 1, rows, rows + WINDOW)
    far_ok = (jnp.abs(q_pos - far_pos) <= WINDOW) & (far_pos >= low_pos) & (far_pos < high_pos)
    far_exp = jnp.where(far_ok, jnp.exp(dot_nt(heads, near_kv[rows:, 0:width])), 0.0)
    total = jnp.sum(own_exp, axis=-1, keepdims=True) + jnp.sum(far_exp, axis=-1, keepdims=True)
    mixed = dot((own_exp / total).astype(BF16), near_kv[0:rows, width:])
    mixed += dot((far_exp / total).astype(BF16), near_kv[rows:, width:])
    joined = mixed[0:rows]
    for h in range(1, n_heads):
        joined = jnp.where(head_lane == h, mixed[h * rows : (h + 1) * rows], joined)
    attended[band] = joined.astype(BF16)
    gather_start(ATT, attended.at[band])

    with jax.named_scope("w_outown"):
        mem_copy(OUT_OWN, out_v.at[band, other]).wait_recv()
    sums = [dot(attended[band], out_v[band, m]) for m in range(2)]
    with jax.named_scope("w_outmem"):
        for q in near_bands:
            mem_copy(OUT_OWN + q, out_v.at[bands[q], other]).wait_recv()
    with jax.named_scope("w_att"):
        for q in near_bands:
            x_wait(ATT, q, attended.at[bands[q]])
    for m in range(2):
        for q in near_bands:
            sums[m] = sums[m] + dot(attended[bands[q]], out_v[bands[q], m])
    stream = stream_v[...] + jnp.concatenate(sums, axis=1)
    stream_v[...] = stream
    normed = rms_norm(stream).astype(BF16)

    with jax.named_scope("w_up"):
        mem_copy(UP, up_v.at[other]).wait_recv()
    deep = up_v.shape[1]
    hidden = gelu(dot(normed[:, :deep], up_v[0]) + dot(normed[:, deep:], up_v[1])).astype(BF16)
    high, low = halves(stream_v[:, pl.ds(pl.multiple_of(band * width, width), width)])
    own_dec = dec_v[band].reshape(width, -1)
    part = dot(hidden, fold_v[0]) + dot(hidden, fold_v[1]) + dot(high, own_dec) + dot(low, own_dec)
    proj[band] = part.astype(BF16)
    gather_start(PROJ, proj.at[band])
    z_sent(0, states)
    for k in range(2):
        hop_copy(k).wait_send()
    passed_on(states, STATES)
    for q in near_bands:
        with jax.named_scope(f"w_proj{q}"):
            x_wait(PROJ, q, proj.at[bands[q]])
        part = part + proj[bands[q]].astype(F32)
    nodes = part.astype(BF16)
    for k in (1, 0):
        outgoing = dot_tn(select[k, 0:rows, 0:span], nodes) + dot_tn(select[k, rows : 2 * rows, 0:span], nodes)
        back_z[k] = outgoing.astype(BF16).reshape(back_z.shape[1:])
        for t in range(half_per):
            p = k * half_per + t
            z_start(1, p, back_z.at[k, t], returned, behind_at(order[p]))
    for copy in sent:
        copy.wait_send()

    with jax.named_scope("w_back"):
        for p in range(per):
            z_wait(1, p, returned)
            pass_on(p, returned, BACKS)
    decoded = 0.0
    for k in range(2):
        decoded += dot(pick[k, :, 0:span], returned[k, 0].reshape(span, -1))
    for k in range(2):
        with jax.named_scope(f"w_xb{k}"):
            for q in near_bands:
                x_wait(BACKS[k], q, returned.at[k, q])
        decoded += dot(pick[k, :, span:], returned[k, 1:].reshape((n_band - 1) * span, -1))
    result = jnp.where(free_v[...] > 0.5, grid_v[...].astype(F32) + decoded, forcing_v[...].astype(F32))
    next_ref[...] = result.astype(BF16)
    z_sent(1, returned)
    passed_on(returned, BACKS)


def body(
    grid_state, forcing, boundary_mask, edge_src, edge_dst, edge_count, edge_weight,
    embed_weight, attn_qkv, attn_out, mlp_in, mlp_out, decode_weight,
):
    n_grid, n_band, n_mem = lax.axis_size("grid"), lax.axis_size("band"), lax.axis_size("mem")
    grid_rows = grid_state[0]
    points, channels = grid_rows.shape
    slots = edge_src.shape[2]
    model = decode_weight.shape[0] * n_band
    width = embed_weight.shape[1]
    rows = M_DEV
    per = n_grid // n_band
    group = per * slots
    operands = (
        grid_rows, forcing, boundary_mask.reshape(-1, channels), edge_src[0], edge_dst, edge_count.T, edge_weight, embed_weight,
        jnp.swapaxes(attn_qkv[0], 0, 1), attn_out[0], mlp_in[0], mlp_out[0], decode_weight,
    )
    vmem = pltpu.VMEM
    spread_over = {7: (n_band,), 8: (n_mem,), 9: (n_band, n_mem), 10: (n_mem,), 11: (n_mem,)}
    scratch = [vmem((*spread_over.get(k, ()), *a.shape), a.dtype) for k, a in enumerate(operands[:12])]
    scratch += [
        vmem((n_band, n_mem, width // n_mem, channels), BF16),
        vmem((2, points, n_band * group // 2), BF16),
        vmem((2, 2 * rows, n_band * group // 2), BF16),
        vmem((points, channels), F32),
        vmem((2, per // 2, slots, channels), BF16),
        vmem((2, per // 4, slots, channels), BF16),
        vmem((2, n_band, per // 2, slots, channels), BF16),
        vmem((rows + 2 * WINDOW, 2 * width), BF16),
        vmem((n_band, rows, width), BF16),
        vmem((rows, model), F32),
        vmem((2, mlp_out.shape[1], channels), BF16),
        vmem((n_band, rows, channels), BF16),
        vmem((2, per // 2, slots, channels), BF16),
        vmem((2, n_band, per // 2, slots, channels), BF16),
        pltpu.SemaphoreType.DMA((14,)),
        pltpu.SemaphoreType.DMA((2, per)),
        pltpu.SemaphoreType.DMA((2, per)),
        pltpu.SemaphoreType.DMA((2,)),
        pltpu.SemaphoreType.DMA((2,)),
        pltpu.SemaphoreType.DMA((len(STAGES), n_band)),
        pltpu.SemaphoreType.DMA((len(STAGES), n_band)),
        pltpu.SemaphoreType.DMA((2 * n_band + 5,)),
        pltpu.SemaphoreType.DMA((2 * n_band + 5,)),
    ]
    result = pl.pallas_call(
        functools.partial(step_kernel, n_grid, n_band, model // HEADS),
        out_shape=pltpu.VMEM((points, channels), BF16),
        in_specs=[pl.BlockSpec(memory_space=pl.ANY)] * len(operands),
        out_specs=pl.BlockSpec(memory_space=pltpu.VMEM),
        scratch_shapes=scratch,
        compiler_params=pltpu.CompilerParams(collective_id=0, has_side_effects=True, vmem_limit_bytes=VMEM_BYTES),
    )(*operands)
    return result[None]


def solution(mesh):
    return jax.shard_map(
        body,
        mesh=mesh,
        in_specs=(
            P(("dom", "mem"), "grid", None),
            P(("dom", "grid"), None),
            P("grid"),
            P("grid", None, None),
            P(None, "grid", None),
            P(None, "grid"),
            P(None, "grid", None),
            P(None, "band"),
            P(None, "mem", None, "band"),
            P(None, "band", "mem"),
            P(None, "mem", "band"),
            P(None, "band", "mem"),
            P("band", None),
        ),
        out_specs=P(("dom", "mem"), "grid", None),
        check_vma=False,
    )
```

```python
import functools
import math

import jax
import jax.numpy as jnp
from jax import lax
from jax.experimental import pallas as pl
from jax.experimental.pallas import tpu as pltpu
from jax.sharding import PartitionSpec as P

HEADS = 16
M_DEV = 128
WINDOW = 64
VMEM_BYTES = 61_500_000
EMBED, OUT, PASS, DEC, ATT, PROJ, *MORE = STAGES = range(12)
STATES, BACKS, CROSSED = MORE[:2], MORE[2:4], MORE[4:]
F32 = jnp.float32
BF16 = jnp.bfloat16
MESH = pl.DeviceIdType.MESH


def dot(left, right):
    return jnp.dot(left, right, preferred_element_type=F32)


def dot_tn(left, right):
    return lax.dot_general(left, right, (((0,), (0,)), ((), ())), preferred_element_type=F32)


def dot_nt(left, right):
    return lax.dot_general(left, right, (((1,), (1,)), ((), ())), preferred_element_type=F32)


def exact_dot(left, right):
    return jnp.dot(left, right, precision=lax.Precision.HIGHEST, preferred_element_type=F32)


def gelu(x):
    scale = math.sqrt(2.0 / math.pi)
    half = 0.5 * x
    return half * jnp.tanh(x * (x * x * (0.044715 * scale) + scale)) + half


def rms_norm(values):
    return values * lax.rsqrt(jnp.mean(values * values, axis=-1, keepdims=True) + 1e-06)


def halves(values):
    high = values.astype(BF16)
    return high, (values - high.astype(F32)).astype(BF16)


def step_kernel(
    n_grid, n_band, head_dim,
    grid_in, forcing_in, mask_in, src_in, dst_in, count_in, weight_in, embed_in, qkv_in, out_in, up_in, down_in, dec_in,
    next_ref,
    grid_v, forcing_v, mask_v, src_v, dst_v, count_v, weight_v, embed_v, qkv_v, out_v, up_v, down_v, dec_v,
    pick, select, free_v, send_z, relayed, states, near_kv, attended, stream_v, fold_v, proj, back_z, returned,
    load_sem, z_send, z_recv, hop_send, hop_recv, x_send, x_recv, mem_send, mem_recv,
):
    me = lax.axis_index("grid")
    band = lax.axis_index("band")
    mem = lax.axis_index("mem")
    other = 1 - mem
    per = n_grid // n_band
    slots = src_v.shape[1]
    group = per * slots
    up_next, down_next = lax.rem(me + 1, n_grid), lax.rem(me + n_grid - 1, n_grid)
    bands = [lax.rem(band + q, n_band) for q in range(n_band)]
    far_bands = sorted(range(1, n_band), key=lambda q: -min(q, n_band - q))
    near_bands = far_bands[::-1]
    beside, across = (1, n_band - 1), n_band // 2
    quarter, half_per = per // 4, per // 2
    order = [*range(quarter), *range(3 * quarter, per), *range(quarter, 3 * quarter)]
    ahead = [lax.rem(bands[q] + 2 * (n_grid - me), n_band) for q in range(n_band)]
    behind = [lax.rem(n_band - a, n_band) for a in ahead]
    is_self = ahead[0] == 0
    reach = n_grid // 4
    hops = (lax.rem(me + reach, n_grid), lax.rem(me + n_grid - reach, n_grid))

    def ahead_at(r):
        return lax.rem(me + ahead[0] + n_band * r, n_grid)

    def behind_at(r):
        return lax.rem(me + 2 * n_grid - behind[0] - n_band * r, n_grid)

    half = dec_v.shape[2]
    loads = [
        pltpu.make_async_copy(source, target, load_sem.at[k])
        for k, (source, target) in enumerate(
            (
                (src_in, src_v), (grid_in, grid_v), (embed_in, embed_v.at[band]),
                (dst_in, dst_v), (count_in, count_v), (weight_in, weight_v), (mask_in, mask_v), (forcing_in, forcing_v),
                (qkv_in, qkv_v.at[mem]), (out_in, out_v.at[band, mem]), (up_in, up_v.at[mem]), (down_in, down_v.at[mem]),
                (dec_in.at[0:half], dec_v.at[band, 0]), (dec_in.at[half : 2 * half], dec_v.at[band, 1]),
            )
        )
    ]
    loads[0].start()
    loads[1].start()

    barrier = pltpu.get_barrier_semaphore()

    def greet(device):
        pl.semaphore_signal(barrier, inc=1, device_id=device, device_id_type=MESH)

    for p in range(half_per)[::-1]:
        if order[p] == 0:
            @pl.when(jnp.logical_not(is_self))
            def _():
                greet({"grid": ahead_at(0)})
        else:
            greet({"grid": ahead_at(order[p])})
    for device in hops:
        greet({"grid": device})
    greet({"grid": up_next})
    greet({"grid": down_next})
    for q in far_bands:
        greet({"band": bands[q]})
    greet({"mem": other})

    for load in loads[2:]:
        load.start()

    span = half_per * slots
    lane = lax.broadcasted_iota(jnp.int32, (slots, span), 1)
    spread = jnp.where(lax.rem(lane, slots) == lax.broadcasted_iota(jnp.int32, (slots, span), 0), 1.0, 0.0).astype(F32)
    shard_row = lax.broadcasted_iota(jnp.int32, (n_grid, span), 0)
    place_lane = lax.broadcasted_iota(jnp.int32, (n_grid, span), 1) // slots
    step_lane = []
    for k in range(2):
        steps = jnp.zeros_like(place_lane)
        for p in range(half_per):
            steps = jnp.where(place_lane == p, n_band * order[k * half_per + p], steps)
        step_lane.append(steps)

    def lane_row(wide, shards):
        mine = shard_row == lax.rem(shards, n_grid)
        return jnp.sum(jnp.where(mine, wide, 0.0), axis=0, keepdims=True)

    point = lax.broadcasted_iota(jnp.int32, (grid_v.shape[0], span), 0).astype(F32)

    def build_pick(k, q):
        row = lane_row(src_wide, me + ahead[q] + step_lane[k])
        pick[k, :, q * span : (q + 1) * span] = jnp.where(point == row, 1.0, 0.0).astype(BF16)

    with jax.named_scope("w_load"):
        loads[0].wait()
        loads[1].wait()
    src_wide = exact_dot(src_v[...].astype(F32), spread)
    for k in range(2):
        build_pick(k, 0)
        send_z[k] = dot_tn(pick[k, :, 0:span], grid_v[...]).astype(BF16).reshape(send_z.shape[1:])

    with jax.named_scope("w_barrier"):
        pl.semaphore_wait(barrier, half_per + 4 + n_band - jnp.where(is_self, 1, 0))

    def at_place(ref, p):
        return ref.at[p // half_per, 0, p % half_per]

    def z_copy(way, p, source, target, device):
        return pltpu.make_async_remote_copy(
            src_ref=source, dst_ref=at_place(target, p), send_sem=z_send.at[way, p], recv_sem=z_recv.at[way, p],
            device_id={"grid": device}, device_id_type=MESH,
        )

    def z_own(way, p, source, target):
        return pltpu.make_async_copy(source, at_place(target, p), z_recv.at[way, p])

    def may_stay(way, p):
        return order[p] == 0 or (way == 0 and order[p] == quarter)

    def each_way(way, p, stay, go):
        if may_stay(way, p):
            if stay is not None:
                @pl.when(is_self)
                def _():
                    stay()

            @pl.when(jnp.logical_not(is_self))
            def _():
                go()
        else:
            go()

    def z_start(way, p, source, target, device):
        each_way(
            way, p, lambda: z_own(way, p, source, target).start(), lambda: z_copy(way, p, source, target, device).start()
        )

    def z_wait(way, p, target):
        here = at_place(target, p)
        each_way(
            way, p, lambda: z_own(way, p, here, target).wait(), lambda: z_copy(way, p, here, target, up_next).wait_recv()
        )

    def z_sent(way, target):
        for p in range(per):
            here = at_place(target, p)
            each_way(way, p, None, lambda: z_copy(way, p, here, target, up_next).wait_send())

    def hop_copy(k):
        return pltpu.make_async_remote_copy(
            src_ref=send_z.at[1, pl.ds(k * quarter, quarter)], dst_ref=relayed.at[k],
            send_sem=hop_send.at[k], recv_sem=hop_recv.at[k], device_id={"grid": hops[k]}, device_id_type=MESH,
        )

    def x_copy(stage, q, source, target):
        return pltpu.make_async_remote_copy(
            src_ref=source, dst_ref=target, send_sem=x_send.at[stage, q], recv_sem=x_recv.at[stage, n_band - q],
            device_id={"band": bands[q]}, device_id_type=MESH,
        )

    def x_wait(stage, q, target):
        pltpu.make_async_remote_copy(
            src_ref=target, dst_ref=target, send_sem=x_send.at[stage, q], recv_sem=x_recv.at[stage, q],
            device_id={"band": bands[q]}, device_id_type=MESH,
        ).wait_recv()

    def mem_copy(k, ref):
        return pltpu.make_async_remote_copy(
            src_ref=ref, dst_ref=ref, send_sem=mem_send.at[k], recv_sem=mem_recv.at[k],
            device_id={"mem": other}, device_id_type=MESH,
        )

    sent = []

    def start(copy):
        copy.start()
        sent.append(copy)

    def gather_start(stage, ref):
        for q in far_bands:
            start(x_copy(stage, q, ref, ref))

    QKV, UP, DOWN, OUT_OWN, DEC_OWN, HALO, CROSS = 0, 1, 2, 3, 3 + n_band, 3 + 2 * n_band, 7 + 2 * n_band

    for k in range(2):
        hop_copy(k).start()
    for p in range(half_per)[::-1]:
        z_start(0, p, send_z.at[0, p], states, ahead_at(order[p]))
    with jax.named_scope("w_load2"):
        loads[2].wait()
    gather_start(EMBED, embed_v.at[band])
    with jax.named_scope("w_load3"):
        for load in loads[3:]:
            load.wait()
    for k, ref in ((QKV, qkv_v), (DOWN, down_v), (UP, up_v)):
        start(mem_copy(k, ref.at[mem]))
    start(mem_copy(OUT_OWN, out_v.at[band, mem]))
    for q in far_bands:
        start(x_copy(DEC, q, dec_v.at[band, mem], dec_v.at[band, mem]))
    for q in beside[: n_band // 2]:
        start(x_copy(OUT, q, out_v.at[band, mem], out_v.at[band, mem]))

    rows = stream_v.shape[0]
    square_row = lax.broadcasted_iota(jnp.int32, (n_grid, n_grid), 0)
    square_lane = lax.broadcasted_iota(jnp.int32, (n_grid, n_grid), 1)
    counts = jnp.sum(jnp.where(square_row == square_lane, count_v[...].astype(F32), 0.0), axis=1, keepdims=True)
    slot_lane = lax.broadcasted_iota(jnp.int32, (n_grid, slots), 1).astype(F32)
    live = jnp.where(slot_lane < counts, weight_v[:, 0, :], 0.0)
    dst_wide = exact_dot(dst_v[:, 0, :].astype(F32), spread)
    live_wide = exact_dot(live, spread)
    node = lax.broadcasted_iota(jnp.int32, (rows, span), 0).astype(F32)

    def build_tables(k):
        for q in range(n_band):
            shards = me + 2 * n_grid - behind[q] - step_lane[k]
            table = jnp.where(node == lane_row(dst_wide, shards), lane_row(live_wide, shards), 0.0)
            high, low = halves(table)
            select[k, 0:rows, q * span : (q + 1) * span] = high
            select[k, rows : 2 * rows, q * span : (q + 1) * span] = low
            if q:
                build_pick(k, q)

    build_tables(0)
    build_tables(1)
    lanes = mask_v.shape[1]
    diagonal = lax.broadcasted_iota(jnp.int32, (lanes, lanes), 0) == lax.broadcasted_iota(jnp.int32, (lanes, lanes), 1)
    for k in range(mask_v.shape[0]):
        flags = jnp.where(mask_v[k : k + 1, :] == 1, 0.0, 1.0).astype(F32)
        column = jnp.sum(jnp.where(diagonal, flags, 0.0), axis=1, keepdims=True)
        free_v[k * lanes : (k + 1) * lanes] = jnp.broadcast_to(column, (lanes, free_v.shape[1]))

    with jax.named_scope("w_hop"):
        for k in range(2):
            hop_copy(k).wait_recv()
            for t in range(quarter):
                z_start(0, half_per + k * quarter + t, relayed.at[k, t], states, ahead_at((0, 3 * quarter)[k] + t))

    def pass_on(p, ref, stages):
        k, t = p // half_per, p % half_per
        for q in far_bands:
            x_copy(stages[k], q, ref.at[k, 0, t], ref.at[k, n_band - q, t]).start()

    def passed_on(ref, stages):
        for k in range(2):
            for q in far_bands:
                x_copy(stages[k], q, ref.at[k, 0], ref.at[k, n_band - q]).wait_send()

    width = embed_v.shape[2]

    def encode(block, table, first=False):
        for col in range(n_band):
            both = dot(table, gelu(dot(block, embed_v[col])).astype(BF16))
            part = both[:rows] + both[rows:]
            cols = slice(col * width, (col + 1) * width)
            stream_v[:, cols] = part if first else stream_v[:, cols] + part

    with jax.named_scope("w_znear"):
        for p in range(half_per):
            z_wait(0, p, states)
            pass_on(p, states, STATES)
    with jax.named_scope("w_zfar"):
        for p in range(half_per, per):
            z_wait(0, p, states)
            pass_on(p, states, STATES)
    out_half = out_v.shape[2] // 2
    with jax.named_scope("w_dec"):
        for q in near_bands:
            x_wait(DEC, q, dec_v.at[bands[q], mem])
            start(mem_copy(DEC_OWN + q, dec_v.at[bands[q], mem]))
    with jax.named_scope("w_out"):
        for k, q in enumerate(beside[: n_band // 2]):
            x_wait(OUT, q, out_v.at[bands[q], mem])
            if n_band > 2:
                piece = out_v.at[bands[q], mem, pl.ds(k * out_half, out_half)]
                start(x_copy(PASS, n_band - q, piece, piece))
            start(mem_copy(OUT_OWN + q, out_v.at[bands[q], mem]))
    with jax.named_scope("w_embed"):
        for q in near_bands:
            x_wait(EMBED, q, embed_v.at[bands[q]])
    own = jnp.concatenate([states[k, 0].reshape(span, -1) for k in range(2)], axis=0)
    encode(own, jnp.concatenate([select[k, :, 0:span] for k in range(2)], axis=1), True)
    with jax.named_scope("w_xnear"):
        for q in near_bands:
            x_wait(STATES[0], q, states.at[0, q])
    encode(states[0, 1:].reshape((n_band - 1) * span, -1), select[0, :, span:])

    half_cols = out_v.shape[3]
    with jax.named_scope("w_down"):
        mem_copy(DOWN, down_v.at[other]).wait_recv()
        for q in near_bands:
            mem_copy(DEC_OWN + q, dec_v.at[bands[q], other]).wait_recv()
    fold = 0.0
    for k in range(n_band):
        per_half = half_cols // width
        columns = slice((k % per_half) * width, (k % per_half + 1) * width)
        fold += dot(down_v[k // per_half, :, columns], dec_v[k].reshape(width, -1))
    high, low = halves(fold)
    fold_v[0] = high
    fold_v[1] = low

    with jax.named_scope("w_xfar"):
        for q in near_bands:
            x_wait(STATES[1], q, states.at[1, q])
    encode(states[1, 1:].reshape((n_band - 1) * span, -1), select[1, :, span:])
    stream = stream_v[...].astype(BF16).astype(F32)
    stream_v[...] = stream
    normed = rms_norm(stream).astype(BF16)

    with jax.named_scope("w_qkv"):
        mem_copy(QKV, qkv_v.at[other]).wait_recv()
    deep = qkv_v.shape[2]

    def project(which):
        return dot(normed[:, :deep], qkv_v[0, which]) + dot(normed[:, deep:], qkv_v[1, which])

    lane_r = lax.broadcasted_iota(jnp.int32, (width, width), 0) // head_dim
    lane_c = lax.broadcasted_iota(jnp.int32, (width, width), 1) // head_dim
    head_mean = jnp.where(lane_r == lane_c, 1.0 / head_dim, 0.0).astype(BF16)

    def head_norm(values):
        high, low = halves(values * values)
        return values * lax.rsqrt(dot(high, head_mean) + dot(low, head_mean) + 1e-06)

    lower, upper = pl.ds(rows, WINDOW), pl.ds(rows + WINDOW, WINDOW)
    both_sides = ((pl.ds(rows - WINDOW, WINDOW), lower, up_next), (pl.ds(0, WINDOW), upper, down_next))

    def halo(which):
        lanes = pl.ds(which * width, width)
        return [
            pltpu.make_async_remote_copy(
                src_ref=near_kv.at[source, lanes], dst_ref=near_kv.at[target, lanes],
                send_sem=mem_send.at[HALO + 2 * which + k], recv_sem=mem_recv.at[HALO + 2 * which + k],
                device_id={"grid": device}, device_id_type=MESH,
            )
            for k, (source, target, device) in enumerate(both_sides)
        ]

    near_kv[0:rows, 0:width] = head_norm(project(1)).astype(BF16)
    key_halo, value_halo = halo(0), halo(1)
    for copy in key_halo:
        copy.start()
    near_kv[0:rows, width:] = project(2).astype(BF16)
    for copy in value_halo:
        copy.start()

    n_heads = width // head_dim
    query = head_norm(project(0)).astype(BF16) * jnp.asarray(head_dim**-0.5, BF16)
    head_lane = lax.broadcasted_iota(jnp.int32, (rows, width), 1) // head_dim
    zero = jnp.zeros_like(query)
    heads = jnp.concatenate([jnp.where(head_lane == h, query, zero) for h in range(n_heads)], axis=0)
    tall = n_heads * rows
    q_pos = lax.rem(lax.broadcasted_iota(jnp.int32, (tall, rows), 0), rows)
    k_pos = lax.broadcasted_iota(jnp.int32, (tall, rows), 1)
    own_scores = dot_nt(heads, near_kv[0:rows, 0:width])
    own_exp = jnp.where(jnp.abs(q_pos - k_pos) <= WINDOW, jnp.exp(own_scores), 0.0)
    if n_band > 2:
        with jax.named_scope("w_pass"):
            for k, q in enumerate(beside):
                x_wait(PASS, q, out_v.at[bands[across], mem, pl.ds(k * out_half, out_half)])
        start(mem_copy(OUT_OWN + across, out_v.at[bands[across], mem]))
    with jax.named_scope("w_halo"):
        for copy in key_halo:
            copy.wait()
    far_pos = jnp.where(k_pos < WINDOW, k_pos - WINDOW, k_pos + rows - WINDOW)
    low_pos = jnp.where(me == 0, 0, -WINDOW)
    high_pos = jnp.where(me == n_grid - 1, rows, rows + WINDOW)
    far_ok = (jnp.abs(q_pos - far_pos) <= WINDOW) & (far_pos >= low_pos) & (far_pos < high_pos)
    far_exp = jnp.where(far_ok, jnp.exp(dot_nt(heads, near_kv[rows:, 0:width])), 0.0)
    total = jnp.sum(own_exp, axis=-1, keepdims=True) + jnp.sum(far_exp, axis=-1, keepdims=True)
    with jax.named_scope("w_halo_v"):
        for copy in value_halo:
            copy.wait()
    mixed = dot((own_exp / total).astype(BF16), near_kv[0:rows, width:])
    mixed += dot((far_exp / total).astype(BF16), near_kv[rows:, width:])
    joined = mixed[0:rows]
    for h in range(1, n_heads):
        joined = jnp.where(head_lane == h, mixed[h * rows : (h + 1) * rows], joined)
    attended[band] = joined.astype(BF16)
    gather_start(ATT, attended.at[band])

    with jax.named_scope("w_outown"):
        mem_copy(OUT_OWN, out_v.at[band, other]).wait_recv()
    sums = [dot(attended[band], out_v[band, m]) for m in range(2)]
    with jax.named_scope("w_outmem"):
        for q in near_bands:
            mem_copy(OUT_OWN + q, out_v.at[bands[q], other]).wait_recv()
    with jax.named_scope("w_att"):
        for q in near_bands:
            x_wait(ATT, q, attended.at[bands[q]])
    for m in range(2):
        for q in near_bands:
            sums[m] = sums[m] + dot(attended[bands[q]], out_v[bands[q], m])
    stream = stream_v[...] + jnp.concatenate(sums, axis=1)
    stream_v[...] = stream
    normed = rms_norm(stream).astype(BF16)

    with jax.named_scope("w_up"):
        mem_copy(UP, up_v.at[other]).wait_recv()
    deep = up_v.shape[1]
    hidden = gelu(dot(normed[:, :deep], up_v[0]) + dot(normed[:, deep:], up_v[1])).astype(BF16)
    high, low = halves(stream_v[:, pl.ds(pl.multiple_of(band * width, width), width)])
    own_dec = dec_v[band].reshape(width, -1)
    part = dot(hidden, fold_v[0]) + dot(hidden, fold_v[1]) + dot(high, own_dec) + dot(low, own_dec)
    proj[band] = part.astype(BF16)
    gather_start(PROJ, proj.at[band])
    z_sent(0, states)
    for k in range(2):
        hop_copy(k).wait_send()
    passed_on(states, STATES)
    for q in near_bands:
        with jax.named_scope(f"w_proj{q}"):
            x_wait(PROJ, q, proj.at[bands[q]])
        part = part + proj[bands[q]].astype(F32)
    nodes = part.astype(BF16)

    passing = mem == 1
    stays = is_self & passing
    guest = n_band

    def back_copy(p, device):
        k, t = p // half_per, p % half_per
        return pltpu.make_async_remote_copy(
            src_ref=back_z.at[k, t], dst_ref=returned.at[k, (1 - mem) * guest, t],
            send_sem=z_send.at[1, p], recv_sem=z_recv.at[2 - mem, p],
            device_id={"grid": device, "mem": 1}, device_id_type=MESH,
        )

    def back_own(p):
        return pltpu.make_async_copy(back_z.at[0, p], returned.at[0, 0, p], z_recv.at[1, p])

    def unless_own(p, go, stay=None):
        if order[p] == 0:
            if stay is not None:
                pl.when(stays)(stay)
            pl.when(jnp.logical_not(stays))(go)
        else:
            go()

    def back_wait(p, slot):
        k, t = p // half_per, p % half_per
        return pltpu.make_async_remote_copy(
            src_ref=back_z.at[k, t], dst_ref=returned.at[k, slot, t],
            send_sem=z_send.at[1, p], recv_sem=z_recv.at[2 if slot else 1, p],
            device_id={"grid": up_next}, device_id_type=MESH,
        )

    def guest_copies(p):
        k, t = p // half_per, p % half_per
        block = returned.at[k, guest, t]
        copies = [
            pltpu.make_async_remote_copy(
                src_ref=block, dst_ref=returned.at[k, n_band - q, t],
                send_sem=x_send.at[CROSSED[k], q], recv_sem=x_recv.at[BACKS[k], n_band - q],
                device_id={"band": bands[q], "mem": 0}, device_id_type=MESH,
            )
            for q in far_bands
        ]
        return copies + [
            pltpu.make_async_remote_copy(
                src_ref=block, dst_ref=returned.at[k, 0, t],
                send_sem=mem_send.at[CROSS + k], recv_sem=mem_recv.at[CROSS + k],
                device_id={"mem": 0}, device_id_type=MESH,
            )
        ]

    def guest_half(k, q):
        whole = returned.at[k, guest]
        if q:
            return pltpu.make_async_remote_copy(
                src_ref=whole, dst_ref=returned.at[k, n_band - q],
                send_sem=x_send.at[CROSSED[k], q], recv_sem=x_recv.at[BACKS[k], n_band - q],
                device_id={"band": bands[q], "mem": 0}, device_id_type=MESH,
            )
        return pltpu.make_async_remote_copy(
            src_ref=whole, dst_ref=returned.at[k, 0], send_sem=mem_send.at[CROSS + k], recv_sem=mem_recv.at[CROSS + k],
            device_id={"mem": 0}, device_id_type=MESH,
        )

    for k in (1, 0):
        outgoing = dot_tn(select[k, 0:rows, 0:span], nodes) + dot_tn(select[k, rows : 2 * rows, 0:span], nodes)
        back_z[k] = outgoing.astype(BF16).reshape(back_z.shape[1:])
        for t in range(half_per):
            p = k * half_per + t
            unless_own(p, lambda: back_copy(p, behind_at(order[p])).start(), lambda: back_own(p).start())
    for copy in sent:
        copy.wait_send()

    @pl.when(passing)
    def _():
        for p in range(per):
            unless_own(p, lambda: back_wait(p, 0).wait_recv(), lambda: back_own(p).wait())
            pass_on(p, returned, BACKS)
        for p in range(per):
            back_wait(p, guest).wait_recv()
            for copy in guest_copies(p):
                copy.start()

    @pl.when(jnp.logical_not(passing))
    def _():
        for k in range(2):
            guest_half(k, 0).wait_recv()

    decoded = 0.0
    for k in range(2):
        decoded += dot(pick[k, :, 0:span], returned[k, 0].reshape(span, -1))
    for k in range(2):
        with jax.named_scope(f"w_xb{k}"):
            for q in near_bands:
                x_wait(BACKS[k], q, returned.at[k, q])
        decoded += dot(pick[k, :, span:], returned[k, 1:n_band].reshape((n_band - 1) * span, -1))
    result = jnp.where(free_v[...] > 0.5, grid_v[...].astype(F32) + decoded, forcing_v[...].astype(F32))
    next_ref[...] = result.astype(BF16)
    for p in range(per):
        unless_own(p, lambda: back_copy(p, behind_at(order[p])).wait_send())

    @pl.when(passing)
    def _():
        passed_on(returned, BACKS)
        for k in range(2):
            for q in range(n_band):
                guest_half(k, q).wait_send()


def body(
    grid_state, forcing, boundary_mask, edge_src, edge_dst, edge_count, edge_weight,
    embed_weight, attn_qkv, attn_out, mlp_in, mlp_out, decode_weight,
):
    n_grid, n_band, n_mem = lax.axis_size("grid"), lax.axis_size("band"), lax.axis_size("mem")
    grid_rows = grid_state[0]
    points, channels = grid_rows.shape
    slots = edge_src.shape[2]
    model = decode_weight.shape[0] * n_band
    width = embed_weight.shape[1]
    rows = M_DEV
    per = n_grid // n_band
    group = per * slots
    operands = (
        grid_rows, forcing, boundary_mask.reshape(-1, channels), edge_src[0], edge_dst, edge_count.T, edge_weight, embed_weight,
        jnp.swapaxes(attn_qkv[0], 0, 1), attn_out[0], mlp_in[0], mlp_out[0], decode_weight,
    )
    vmem = pltpu.VMEM
    spread_over = {7: (n_band,), 8: (n_mem,), 9: (n_band, n_mem), 10: (n_mem,), 11: (n_mem,)}
    scratch = [vmem((*spread_over.get(k, ()), *a.shape), a.dtype) for k, a in enumerate(operands[:12])]
    scratch += [
        vmem((n_band, n_mem, width // n_mem, channels), BF16),
        vmem((2, points, n_band * group // 2), BF16),
        vmem((2, 2 * rows, n_band * group // 2), BF16),
        vmem((points, channels), F32),
        vmem((2, per // 2, slots, channels), BF16),
        vmem((2, per // 4, slots, channels), BF16),
        vmem((2, n_band, per // 2, slots, channels), BF16),
        vmem((rows + 2 * WINDOW, 2 * width), BF16),
        vmem((n_band, rows, width), BF16),
        vmem((rows, model), F32),
        vmem((2, mlp_out.shape[1], channels), BF16),
        vmem((n_band, rows, channels), BF16),
        vmem((2, per // 2, slots, channels), BF16),
        vmem((2, n_band + 1, per // 2, slots, channels), BF16),
        pltpu.SemaphoreType.DMA((14,)),
        pltpu.SemaphoreType.DMA((2, per)),
        pltpu.SemaphoreType.DMA((3, per)),
        pltpu.SemaphoreType.DMA((2,)),
        pltpu.SemaphoreType.DMA((2,)),
        pltpu.SemaphoreType.DMA((len(STAGES), n_band)),
        pltpu.SemaphoreType.DMA((len(STAGES), n_band)),
        pltpu.SemaphoreType.DMA((2 * n_band + 9,)),
        pltpu.SemaphoreType.DMA((2 * n_band + 9,)),
    ]
    result = pl.pallas_call(
        functools.partial(step_kernel, n_grid, n_band, model // HEADS),
        out_shape=pltpu.VMEM((points, channels), BF16),
        in_specs=[pl.BlockSpec(memory_space=pl.ANY)] * len(operands),
        out_specs=pl.BlockSpec(memory_space=pltpu.VMEM),
        scratch_shapes=scratch,
        compiler_params=pltpu.CompilerParams(collective_id=0, has_side_effects=True, vmem_limit_bytes=VMEM_BYTES),
    )(*operands)
    return result[None]


def solution(mesh):
    return jax.shard_map(
        body,
        mesh=mesh,
        in_specs=(
            P(("dom", "mem"), "grid", None),
            P(("dom", "grid"), None),
            P("grid"),
            P("grid", None, None),
            P(None, "grid", None),
            P(None, "grid"),
            P(None, "grid", None),
            P(None, "band"),
            P(None, "mem", None, "band"),
            P(None, "band", "mem"),
            P(None, "mem", "band"),
            P(None, "band", "mem"),
            P("band", None),
        ),
        out_specs=P(("dom", "mem"), "grid", None),
        check_vma=False,
    )
```

```python
import functools
import math

import jax
import jax.numpy as jnp
from jax import lax
from jax.experimental import pallas as pl
from jax.experimental.pallas import tpu as pltpu
from jax.sharding import PartitionSpec as P

HEADS = 16
M_DEV = 128
WINDOW = 64
VMEM_BYTES = 61_500_000
EMBED, OUT, PASS, DEC, ATT, PROJ, *MORE = STAGES = range(12)
STATES, BACKS, CROSSED = MORE[:2], MORE[2:4], MORE[4:]
F32 = jnp.float32
BF16 = jnp.bfloat16
MESH = pl.DeviceIdType.MESH


def dot(left, right):
    return jnp.dot(left, right, preferred_element_type=F32)


def dot_tn(left, right):
    return lax.dot_general(left, right, (((0,), (0,)), ((), ())), preferred_element_type=F32)


def dot_nt(left, right):
    return lax.dot_general(left, right, (((1,), (1,)), ((), ())), preferred_element_type=F32)


def exact_dot(left, right):
    return jnp.dot(left, right, precision=lax.Precision.HIGHEST, preferred_element_type=F32)


def gelu(x):
    scale = math.sqrt(2.0 / math.pi)
    half = 0.5 * x
    return half * jnp.tanh(x * (x * x * (0.044715 * scale) + scale)) + half


def rms_norm(values):
    return values * lax.rsqrt(jnp.mean(values * values, axis=-1, keepdims=True) + 1e-06)


def halves(values):
    high = values.astype(BF16)
    return high, (values - high.astype(F32)).astype(BF16)


def step_kernel(
    n_grid, n_band, head_dim,
    grid_in, forcing_in, mask_in, src_in, dst_in, count_in, weight_in, embed_in, qkv_in, out_in, up_in, down_in, dec_in,
    next_ref,
    grid_v, forcing_v, mask_v, src_v, dst_v, count_v, weight_v, embed_v, qkv_v, out_v, up_v, down_v, dec_v,
    pick, select, free_v, send_z, relayed, states, near_kv, attended, stream_v, fold_v, proj, back_z, returned,
    load_sem, z_send, z_recv, hop_send, hop_recv, x_send, x_recv, mem_send, mem_recv,
):
    me = lax.axis_index("grid")
    band = lax.axis_index("band")
    mem = lax.axis_index("mem")
    other = 1 - mem
    per = n_grid // n_band
    slots = src_v.shape[1]
    group = per * slots
    up_next, down_next = lax.rem(me + 1, n_grid), lax.rem(me + n_grid - 1, n_grid)
    bands = [lax.rem(band + q, n_band) for q in range(n_band)]
    far_bands = sorted(range(1, n_band), key=lambda q: -min(q, n_band - q))
    near_bands = far_bands[::-1]
    beside, across = (1, n_band - 1), n_band // 2
    quarter, half_per = per // 4, per // 2
    order = [*range(quarter), *range(3 * quarter, per), *range(quarter, 3 * quarter)]
    ahead = [lax.rem(bands[q] + 2 * (n_grid - me), n_band) for q in range(n_band)]
    behind = [lax.rem(n_band - a, n_band) for a in ahead]
    is_self = ahead[0] == 0
    reach = n_grid // 4
    hops = (lax.rem(me + reach, n_grid), lax.rem(me + n_grid - reach, n_grid))

    def ahead_at(r):
        return lax.rem(me + ahead[0] + n_band * r, n_grid)

    def behind_at(r):
        return lax.rem(me + 2 * n_grid - behind[0] - n_band * r, n_grid)

    half = dec_v.shape[2]
    loads = [
        pltpu.make_async_copy(source, target, load_sem.at[k])
        for k, (source, target) in enumerate(
            (
                (src_in, src_v), (grid_in, grid_v), (embed_in, embed_v.at[band]),
                (dst_in, dst_v), (count_in, count_v), (weight_in, weight_v), (mask_in, mask_v), (forcing_in, forcing_v),
                (qkv_in, qkv_v.at[mem]), (out_in, out_v.at[band, mem]), (up_in, up_v.at[mem]), (down_in, down_v.at[mem]),
                (dec_in.at[0:half], dec_v.at[band, 0]), (dec_in.at[half : 2 * half], dec_v.at[band, 1]),
            )
        )
    ]
    loads[0].start()
    loads[1].start()

    barrier = pltpu.get_barrier_semaphore()

    def greet(device):
        pl.semaphore_signal(barrier, inc=1, device_id=device, device_id_type=MESH)

    for p in range(half_per)[::-1]:
        if order[p] == 0:
            @pl.when(jnp.logical_not(is_self))
            def _():
                greet({"grid": ahead_at(0)})
        else:
            greet({"grid": ahead_at(order[p])})
    for device in hops:
        greet({"grid": device})
    greet({"grid": up_next})
    greet({"grid": down_next})
    for q in far_bands:
        greet({"band": bands[q]})
    greet({"mem": other})

    for load in loads[2:]:
        load.start()

    span = half_per * slots
    lane = lax.broadcasted_iota(jnp.int32, (slots, span), 1)
    spread = jnp.where(lax.rem(lane, slots) == lax.broadcasted_iota(jnp.int32, (slots, span), 0), 1.0, 0.0).astype(F32)
    shard_row = lax.broadcasted_iota(jnp.int32, (n_grid, span), 0)
    place_lane = lax.broadcasted_iota(jnp.int32, (n_grid, span), 1) // slots
    step_lane = []
    for k in range(2):
        steps = jnp.zeros_like(place_lane)
        for p in range(half_per):
            steps = jnp.where(place_lane == p, n_band * order[k * half_per + p], steps)
        step_lane.append(steps)

    def lane_row(wide, shards):
        mine = shard_row == lax.rem(shards, n_grid)
        return jnp.sum(jnp.where(mine, wide, 0.0), axis=0, keepdims=True)

    point = lax.broadcasted_iota(jnp.int32, (grid_v.shape[0], span), 0).astype(F32)

    def build_pick(k, q):
        row = lane_row(src_wide, me + ahead[q] + step_lane[k])
        pick[k, :, q * span : (q + 1) * span] = jnp.where(point == row, 1.0, 0.0).astype(BF16)

    with jax.named_scope("w_load"):
        loads[0].wait()
        loads[1].wait()
    src_wide = exact_dot(src_v[...].astype(F32), spread)
    for k in range(2):
        build_pick(k, 0)
        send_z[k] = dot_tn(pick[k, :, 0:span], grid_v[...]).astype(BF16).reshape(send_z.shape[1:])

    with jax.named_scope("w_barrier"):
        pl.semaphore_wait(barrier, half_per + 4 + n_band - jnp.where(is_self, 1, 0))

    def at_place(ref, p):
        return ref.at[p // half_per, 0, p % half_per]

    def z_copy(way, p, source, target, device):
        return pltpu.make_async_remote_copy(
            src_ref=source, dst_ref=at_place(target, p), send_sem=z_send.at[way, p], recv_sem=z_recv.at[way, p],
            device_id={"grid": device}, device_id_type=MESH,
        )

    def z_own(way, p, source, target):
        return pltpu.make_async_copy(source, at_place(target, p), z_recv.at[way, p])

    def may_stay(way, p):
        return order[p] == 0 or (way == 0 and order[p] == quarter)

    def each_way(way, p, stay, go):
        if may_stay(way, p):
            if stay is not None:
                @pl.when(is_self)
                def _():
                    stay()

            @pl.when(jnp.logical_not(is_self))
            def _():
                go()
        else:
            go()

    def z_start(way, p, source, target, device):
        each_way(
            way, p, lambda: z_own(way, p, source, target).start(), lambda: z_copy(way, p, source, target, device).start()
        )

    def z_wait(way, p, target):
        here = at_place(target, p)
        each_way(
            way, p, lambda: z_own(way, p, here, target).wait(), lambda: z_copy(way, p, here, target, up_next).wait_recv()
        )

    def z_sent(way, target):
        for p in range(per):
            here = at_place(target, p)
            each_way(way, p, None, lambda: z_copy(way, p, here, target, up_next).wait_send())

    def hop_copy(k):
        return pltpu.make_async_remote_copy(
            src_ref=send_z.at[1, pl.ds(k * quarter, quarter)], dst_ref=relayed.at[k],
            send_sem=hop_send.at[k], recv_sem=hop_recv.at[k], device_id={"grid": hops[k]}, device_id_type=MESH,
        )

    def x_copy(stage, q, source, target):
        return pltpu.make_async_remote_copy(
            src_ref=source, dst_ref=target, send_sem=x_send.at[stage, q], recv_sem=x_recv.at[stage, n_band - q],
            device_id={"band": bands[q]}, device_id_type=MESH,
        )

    def x_wait(stage, q, target):
        pltpu.make_async_remote_copy(
            src_ref=target, dst_ref=target, send_sem=x_send.at[stage, q], recv_sem=x_recv.at[stage, q],
            device_id={"band": bands[q]}, device_id_type=MESH,
        ).wait_recv()

    def mem_copy(k, ref):
        return pltpu.make_async_remote_copy(
            src_ref=ref, dst_ref=ref, send_sem=mem_send.at[k], recv_sem=mem_recv.at[k],
            device_id={"mem": other}, device_id_type=MESH,
        )

    sent = []

    def start(copy):
        copy.start()
        sent.append(copy)

    def gather_start(stage, ref):
        for q in far_bands:
            start(x_copy(stage, q, ref, ref))

    QKV, UP, DOWN, OUT_OWN, DEC_OWN, HALO, CROSS = 0, 1, 2, 3, 3 + n_band, 3 + 2 * n_band, 7 + 2 * n_band

    for k in range(2):
        hop_copy(k).start()
    for p in range(half_per)[::-1]:
        z_start(0, p, send_z.at[0, p], states, ahead_at(order[p]))
    with jax.named_scope("w_load2"):
        loads[2].wait()
    gather_start(EMBED, embed_v.at[band])
    with jax.named_scope("w_load3"):
        for load in loads[3:]:
            load.wait()
    for k, ref in ((QKV, qkv_v), (DOWN, down_v), (UP, up_v)):
        start(mem_copy(k, ref.at[mem]))
    start(mem_copy(OUT_OWN, out_v.at[band, mem]))
    for q in far_bands:
        start(x_copy(DEC, q, dec_v.at[band, mem], dec_v.at[band, mem]))
    for q in beside[: n_band // 2]:
        start(x_copy(OUT, q, out_v.at[band, mem], out_v.at[band, mem]))

    rows = stream_v.shape[0]
    square_row = lax.broadcasted_iota(jnp.int32, (n_grid, n_grid), 0)
    square_lane = lax.broadcasted_iota(jnp.int32, (n_grid, n_grid), 1)
    counts = jnp.sum(jnp.where(square_row == square_lane, count_v[...].astype(F32), 0.0), axis=1, keepdims=True)
    slot_lane = lax.broadcasted_iota(jnp.int32, (n_grid, slots), 1).astype(F32)
    live = jnp.where(slot_lane < counts, weight_v[:, 0, :], 0.0)
    dst_wide = exact_dot(dst_v[:, 0, :].astype(F32), spread)
    live_wide = exact_dot(live, spread)
    node = lax.broadcasted_iota(jnp.int32, (rows, span), 0).astype(F32)

    def build_tables(k):
        for q in range(n_band):
            shards = me + 2 * n_grid - behind[q] - step_lane[k]
            table = jnp.where(node == lane_row(dst_wide, shards), lane_row(live_wide, shards), 0.0)
            high, low = halves(table)
            select[k, 0:rows, q * span : (q + 1) * span] = high
            select[k, rows : 2 * rows, q * span : (q + 1) * span] = low
            if q:
                build_pick(k, q)

    build_tables(0)
    build_tables(1)
    lanes = mask_v.shape[1]
    diagonal = lax.broadcasted_iota(jnp.int32, (lanes, lanes), 0) == lax.broadcasted_iota(jnp.int32, (lanes, lanes), 1)
    for k in range(mask_v.shape[0]):
        flags = jnp.where(mask_v[k : k + 1, :] == 1, 0.0, 1.0).astype(F32)
        column = jnp.sum(jnp.where(diagonal, flags, 0.0), axis=1, keepdims=True)
        free_v[k * lanes : (k + 1) * lanes] = jnp.broadcast_to(column, (lanes, free_v.shape[1]))

    def forward(k):
        hop_copy(k).wait_recv()
        for t in range(quarter):
            z_start(0, half_per + k * quarter + t, relayed.at[k, t], states, ahead_at((0, 3 * quarter)[k] + t))

    with jax.named_scope("w_hop"):
        @pl.when(me < reach)
        def _():
            forward(1)
            forward(0)

        @pl.when(me >= reach)
        def _():
            forward(0)
            forward(1)

    def pass_on(p, ref, stages):
        k, t = p // half_per, p % half_per
        for q in far_bands:
            x_copy(stages[k], q, ref.at[k, 0, t], ref.at[k, n_band - q, t]).start()

    def passed_on(ref, stages):
        for k in range(2):
            for q in far_bands:
                x_copy(stages[k], q, ref.at[k, 0], ref.at[k, n_band - q]).wait_send()

    width = embed_v.shape[2]

    def encode(block, table, first=False):
        for col in range(n_band):
            both = dot(table, gelu(dot(block, embed_v[col])).astype(BF16))
            part = both[:rows] + both[rows:]
            cols = slice(col * width, (col + 1) * width)
            stream_v[:, cols] = part if first else stream_v[:, cols] + part

    with jax.named_scope("w_znear"):
        for p in range(half_per):
            z_wait(0, p, states)
            pass_on(p, states, STATES)
    with jax.named_scope("w_zfar"):
        for p in range(half_per, per):
            z_wait(0, p, states)
            pass_on(p, states, STATES)
    out_half = out_v.shape[2] // 2
    with jax.named_scope("w_dec"):
        for q in near_bands:
            x_wait(DEC, q, dec_v.at[bands[q], mem])
            start(mem_copy(DEC_OWN + q, dec_v.at[bands[q], mem]))
    with jax.named_scope("w_out"):
        for k, q in enumerate(beside[: n_band // 2]):
            x_wait(OUT, q, out_v.at[bands[q], mem])
            if n_band > 2:
                piece = out_v.at[bands[q], mem, pl.ds(k * out_half, out_half)]
                start(x_copy(PASS, n_band - q, piece, piece))
            start(mem_copy(OUT_OWN + q, out_v.at[bands[q], mem]))
    with jax.named_scope("w_embed"):
        for q in near_bands:
            x_wait(EMBED, q, embed_v.at[bands[q]])
    own = jnp.concatenate([states[k, 0].reshape(span, -1) for k in range(2)], axis=0)
    encode(own, jnp.concatenate([select[k, :, 0:span] for k in range(2)], axis=1), True)
    with jax.named_scope("w_xnear"):
        for q in near_bands:
            x_wait(STATES[0], q, states.at[0, q])
    encode(states[0, 1:].reshape((n_band - 1) * span, -1), select[0, :, span:])

    half_cols = out_v.shape[3]
    with jax.named_scope("w_down"):
        mem_copy(DOWN, down_v.at[other]).wait_recv()
        for q in near_bands:
            mem_copy(DEC_OWN + q, dec_v.at[bands[q], other]).wait_recv()
    fold = 0.0
    for k in range(n_band):
        per_half = half_cols // width
        columns = slice((k % per_half) * width, (k % per_half + 1) * width)
        fold += dot(down_v[k // per_half, :, columns], dec_v[k].reshape(width, -1))
    high, low = halves(fold)
    fold_v[0] = high
    fold_v[1] = low

    with jax.named_scope("w_xfar"):
        for q in near_bands:
            x_wait(STATES[1], q, states.at[1, q])
    encode(states[1, 1:].reshape((n_band - 1) * span, -1), select[1, :, span:])
    stream = stream_v[...].astype(BF16).astype(F32)
    stream_v[...] = stream
    normed = rms_norm(stream).astype(BF16)

    with jax.named_scope("w_qkv"):
        mem_copy(QKV, qkv_v.at[other]).wait_recv()
    deep = qkv_v.shape[2]

    def project(which):
        return dot(normed[:, :deep], qkv_v[0, which]) + dot(normed[:, deep:], qkv_v[1, which])

    lane_r = lax.broadcasted_iota(jnp.int32, (width, width), 0) // head_dim
    lane_c = lax.broadcasted_iota(jnp.int32, (width, width), 1) // head_dim
    head_mean = jnp.where(lane_r == lane_c, 1.0 / head_dim, 0.0).astype(BF16)

    def head_norm(values):
        high, low = halves(values * values)
        return values * lax.rsqrt(dot(high, head_mean) + dot(low, head_mean) + 1e-06)

    lower, upper = pl.ds(rows, WINDOW), pl.ds(rows + WINDOW, WINDOW)
    both_sides = ((pl.ds(rows - WINDOW, WINDOW), lower, up_next), (pl.ds(0, WINDOW), upper, down_next))

    def halo(which):
        lanes = pl.ds(which * width, width)
        return [
            pltpu.make_async_remote_copy(
                src_ref=near_kv.at[source, lanes], dst_ref=near_kv.at[target, lanes],
                send_sem=mem_send.at[HALO + 2 * which + k], recv_sem=mem_recv.at[HALO + 2 * which + k],
                device_id={"grid": device}, device_id_type=MESH,
            )
            for k, (source, target, device) in enumerate(both_sides)
        ]

    near_kv[0:rows, 0:width] = head_norm(project(1)).astype(BF16)
    key_halo, value_halo = halo(0), halo(1)
    for copy in key_halo:
        copy.start()
    near_kv[0:rows, width:] = project(2).astype(BF16)
    for copy in value_halo:
        copy.start()

    n_heads = width // head_dim
    query = head_norm(project(0)).astype(BF16) * jnp.asarray(head_dim**-0.5, BF16)
    head_lane = lax.broadcasted_iota(jnp.int32, (rows, width), 1) // head_dim
    zero = jnp.zeros_like(query)
    heads = jnp.concatenate([jnp.where(head_lane == h, query, zero) for h in range(n_heads)], axis=0)
    tall = n_heads * rows
    q_pos = lax.rem(lax.broadcasted_iota(jnp.int32, (tall, rows), 0), rows)
    k_pos = lax.broadcasted_iota(jnp.int32, (tall, rows), 1)
    own_scores = dot_nt(heads, near_kv[0:rows, 0:width])
    own_exp = jnp.where(jnp.abs(q_pos - k_pos) <= WINDOW, jnp.exp(own_scores), 0.0)
    if n_band > 2:
        with jax.named_scope("w_pass"):
            for k, q in enumerate(beside):
                x_wait(PASS, q, out_v.at[bands[across], mem, pl.ds(k * out_half, out_half)])
        start(mem_copy(OUT_OWN + across, out_v.at[bands[across], mem]))
    with jax.named_scope("w_halo"):
        for copy in key_halo:
            copy.wait()
    far_pos = jnp.where(k_pos < WINDOW, k_pos - WINDOW, k_pos + rows - WINDOW)
    low_pos = jnp.where(me == 0, 0, -WINDOW)
    high_pos = jnp.where(me == n_grid - 1, rows, rows + WINDOW)
    far_ok = (jnp.abs(q_pos - far_pos) <= WINDOW) & (far_pos >= low_pos) & (far_pos < high_pos)
    far_exp = jnp.where(far_ok, jnp.exp(dot_nt(heads, near_kv[rows:, 0:width])), 0.0)
    total = jnp.sum(own_exp, axis=-1, keepdims=True) + jnp.sum(far_exp, axis=-1, keepdims=True)
    with jax.named_scope("w_halo_v"):
        for copy in value_halo:
            copy.wait()
    mixed = dot((own_exp / total).astype(BF16), near_kv[0:rows, width:])
    mixed += dot((far_exp / total).astype(BF16), near_kv[rows:, width:])
    joined = mixed[0:rows]
    for h in range(1, n_heads):
        joined = jnp.where(head_lane == h, mixed[h * rows : (h + 1) * rows], joined)
    attended[band] = joined.astype(BF16)
    gather_start(ATT, attended.at[band])

    with jax.named_scope("w_outown"):
        mem_copy(OUT_OWN, out_v.at[band, other]).wait_recv()
    sums = [dot(attended[band], out_v[band, m]) for m in range(2)]
    with jax.named_scope("w_outmem"):
        for q in near_bands:
            mem_copy(OUT_OWN + q, out_v.at[bands[q], other]).wait_recv()
    with jax.named_scope("w_att"):
        for q in near_bands:
            x_wait(ATT, q, attended.at[bands[q]])
    for m in range(2):
        for q in near_bands:
            sums[m] = sums[m] + dot(attended[bands[q]], out_v[bands[q], m])
    stream = stream_v[...] + jnp.concatenate(sums, axis=1)
    stream_v[...] = stream
    normed = rms_norm(stream).astype(BF16)

    with jax.named_scope("w_up"):
        mem_copy(UP, up_v.at[other]).wait_recv()
    deep = up_v.shape[1]
    hidden = gelu(dot(normed[:, :deep], up_v[0]) + dot(normed[:, deep:], up_v[1])).astype(BF16)
    high, low = halves(stream_v[:, pl.ds(pl.multiple_of(band * width, width), width)])
    own_dec = dec_v[band].reshape(width, -1)
    part = dot(hidden, fold_v[0]) + dot(hidden, fold_v[1]) + dot(high, own_dec) + dot(low, own_dec)
    proj[band] = part.astype(BF16)
    gather_start(PROJ, proj.at[band])
    z_sent(0, states)
    for k in range(2):
        hop_copy(k).wait_send()
    passed_on(states, STATES)
    for q in near_bands:
        with jax.named_scope(f"w_proj{q}"):
            x_wait(PROJ, q, proj.at[bands[q]])
        part = part + proj[bands[q]].astype(F32)
    nodes = part.astype(BF16)

    passing = mem == 1
    stays = is_self & passing
    guest = n_band

    def back_copy(p, device):
        k, t = p // half_per, p % half_per
        return pltpu.make_async_remote_copy(
            src_ref=back_z.at[k, t], dst_ref=returned.at[k, (1 - mem) * guest, t],
            send_sem=z_send.at[1, p], recv_sem=z_recv.at[2 - mem, p],
            device_id={"grid": device, "mem": 1}, device_id_type=MESH,
        )

    def back_own(p):
        return pltpu.make_async_copy(back_z.at[0, p], returned.at[0, 0, p], z_recv.at[1, p])

    def unless_own(p, go, stay=None):
        if order[p] == 0:
            if stay is not None:
                pl.when(stays)(stay)
            pl.when(jnp.logical_not(stays))(go)
        else:
            go()

    def back_wait(p, slot):
        k, t = p // half_per, p % half_per
        return pltpu.make_async_remote_copy(
            src_ref=back_z.at[k, t], dst_ref=returned.at[k, slot, t],
            send_sem=z_send.at[1, p], recv_sem=z_recv.at[2 if slot else 1, p],
            device_id={"grid": up_next}, device_id_type=MESH,
        )

    def guest_copies(p):
        k, t = p // half_per, p % half_per
        block = returned.at[k, guest, t]
        copies = [
            pltpu.make_async_remote_copy(
                src_ref=block, dst_ref=returned.at[k, n_band - q, t],
                send_sem=x_send.at[CROSSED[k], q], recv_sem=x_recv.at[BACKS[k], n_band - q],
                device_id={"band": bands[q], "mem": 0}, device_id_type=MESH,
            )
            for q in far_bands
        ]
        return copies + [
            pltpu.make_async_remote_copy(
                src_ref=block, dst_ref=returned.at[k, 0, t],
                send_sem=mem_send.at[CROSS + k], recv_sem=mem_recv.at[CROSS + k],
                device_id={"mem": 0}, device_id_type=MESH,
            )
        ]

    def guest_half(k, q):
        whole = returned.at[k, guest]
        if q:
            return pltpu.make_async_remote_copy(
                src_ref=whole, dst_ref=returned.at[k, n_band - q],
                send_sem=x_send.at[CROSSED[k], q], recv_sem=x_recv.at[BACKS[k], n_band - q],
                device_id={"band": bands[q], "mem": 0}, device_id_type=MESH,
            )
        return pltpu.make_async_remote_copy(
            src_ref=whole, dst_ref=returned.at[k, 0], send_sem=mem_send.at[CROSS + k], recv_sem=mem_recv.at[CROSS + k],
            device_id={"mem": 0}, device_id_type=MESH,
        )

    for k in (1, 0):
        outgoing = dot_tn(select[k, 0:rows, 0:span], nodes) + dot_tn(select[k, rows : 2 * rows, 0:span], nodes)
        back_z[k] = outgoing.astype(BF16).reshape(back_z.shape[1:])
        for t in range(half_per):
            p = k * half_per + t
            unless_own(p, lambda: back_copy(p, behind_at(order[p])).start(), lambda: back_own(p).start())
    for copy in sent:
        copy.wait_send()

    @pl.when(passing)
    def _():
        for p in range(per):
            unless_own(p, lambda: back_wait(p, 0).wait_recv(), lambda: back_own(p).wait())
            pass_on(p, returned, BACKS)
        for p in range(per):
            back_wait(p, guest).wait_recv()
            for copy in guest_copies(p):
                copy.start()

    @pl.when(jnp.logical_not(passing))
    def _():
        for k in range(2):
            guest_half(k, 0).wait_recv()

    decoded = 0.0
    for k in range(2):
        decoded += dot(pick[k, :, 0:span], returned[k, 0].reshape(span, -1))
    for k in range(2):
        with jax.named_scope(f"w_xb{k}"):
            for q in near_bands:
                x_wait(BACKS[k], q, returned.at[k, q])
        decoded += dot(pick[k, :, span:], returned[k, 1:n_band].reshape((n_band - 1) * span, -1))
    result = jnp.where(free_v[...] > 0.5, grid_v[...].astype(F32) + decoded, forcing_v[...].astype(F32))
    next_ref[...] = result.astype(BF16)
    for p in range(per):
        unless_own(p, lambda: back_copy(p, behind_at(order[p])).wait_send())

    @pl.when(passing)
    def _():
        passed_on(returned, BACKS)
        for k in range(2):
            for q in range(n_band):
                guest_half(k, q).wait_send()


def body(
    grid_state, forcing, boundary_mask, edge_src, edge_dst, edge_count, edge_weight,
    embed_weight, attn_qkv, attn_out, mlp_in, mlp_out, decode_weight,
):
    n_grid, n_band, n_mem = lax.axis_size("grid"), lax.axis_size("band"), lax.axis_size("mem")
    grid_rows = grid_state[0]
    points, channels = grid_rows.shape
    slots = edge_src.shape[2]
    model = decode_weight.shape[0] * n_band
    width = embed_weight.shape[1]
    rows = M_DEV
    per = n_grid // n_band
    group = per * slots
    operands = (
        grid_rows, forcing, boundary_mask.reshape(-1, channels), edge_src[0], edge_dst, edge_count.T, edge_weight, embed_weight,
        jnp.swapaxes(attn_qkv[0], 0, 1), attn_out[0], mlp_in[0], mlp_out[0], decode_weight,
    )
    vmem = pltpu.VMEM
    spread_over = {7: (n_band,), 8: (n_mem,), 9: (n_band, n_mem), 10: (n_mem,), 11: (n_mem,)}
    scratch = [vmem((*spread_over.get(k, ()), *a.shape), a.dtype) for k, a in enumerate(operands[:12])]
    scratch += [
        vmem((n_band, n_mem, width // n_mem, channels), BF16),
        vmem((2, points, n_band * group // 2), BF16),
        vmem((2, 2 * rows, n_band * group // 2), BF16),
        vmem((points, channels), F32),
        vmem((2, per // 2, slots, channels), BF16),
        vmem((2, per // 4, slots, channels), BF16),
        vmem((2, n_band, per // 2, slots, channels), BF16),
        vmem((rows + 2 * WINDOW, 2 * width), BF16),
        vmem((n_band, rows, width), BF16),
        vmem((rows, model), F32),
        vmem((2, mlp_out.shape[1], channels), BF16),
        vmem((n_band, rows, channels), BF16),
        vmem((2, per // 2, slots, channels), BF16),
        vmem((2, n_band + 1, per // 2, slots, channels), BF16),
        pltpu.SemaphoreType.DMA((14,)),
        pltpu.SemaphoreType.DMA((2, per)),
        pltpu.SemaphoreType.DMA((3, per)),
        pltpu.SemaphoreType.DMA((2,)),
        pltpu.SemaphoreType.DMA((2,)),
        pltpu.SemaphoreType.DMA((len(STAGES), n_band)),
        pltpu.SemaphoreType.DMA((len(STAGES), n_band)),
        pltpu.SemaphoreType.DMA((2 * n_band + 9,)),
        pltpu.SemaphoreType.DMA((2 * n_band + 9,)),
    ]
    result = pl.pallas_call(
        functools.partial(step_kernel, n_grid, n_band, model // HEADS),
        out_shape=pltpu.VMEM((points, channels), BF16),
        in_specs=[pl.BlockSpec(memory_space=pl.ANY)] * len(operands),
        out_specs=pl.BlockSpec(memory_space=pltpu.VMEM),
        scratch_shapes=scratch,
        compiler_params=pltpu.CompilerParams(collective_id=0, has_side_effects=True, vmem_limit_bytes=VMEM_BYTES),
    )(*operands)
    return result[None]


def solution(mesh):
    return jax.shard_map(
        body,
        mesh=mesh,
        in_specs=(
            P(("dom", "mem"), "grid", None),
            P(("dom", "grid"), None),
            P("grid"),
            P("grid", None, None),
            P(None, "grid", None),
            P(None, "grid"),
            P(None, "grid", None),
            P(None, "band"),
            P(None, "mem", None, "band"),
            P(None, "band", "mem"),
            P(None, "mem", "band"),
            P(None, "band", "mem"),
            P("band", None),
        ),
        out_specs=P(("dom", "mem"), "grid", None),
        check_vma=False,
    )
```
